32 devices in a mesh: sx: 4 (over y, x), sy: 8 (over z, core).
Axes of the slice: x: 2, y: 2, z: 4, core: 2. Of those that a mesh axis runs over, the one named last changes fastest.
Arguments:
- collocation: float32 [2, 4, 2048], P(None, 'sx', 'sy'), may hold values from -1 to 1
- source: float32 [4, 2048], P('sx', 'sy'), may hold values from -31.5 to 40.5
- wall_index: int32 [4, 4, 512], P(None, 'sx', 'sy'), may hold values from 0 to 1023, as said below
- bc_type: int32 [2, 8], P(None, 'sy'), may hold values from 0 to 1
- bc_value: float32 [2, 512], P(None, 'sy'), may hold values from -4 to 4
- in_weight: float32 [4, 3, 4096], P('sx', None, 'sy'), may hold values from -4 to 4
- local_weight: bfloat16 [4, 512, 4096], P('sx', None, 'sy'), may hold values from -0.25 to 0.25
- local_bias: float32 [4, 4096], P('sx', 'sy'), may hold values from -3 to 3
- trunk_weight: bfloat16 [1, 512, 512], replicated, may hold values from -0.25 to 0.25
- trunk_bias: float32 [1, 512], replicated, may hold values from -3 to 3
- head_weight: float32 [4, 4096], P('sx', 'sy'), may hold values from -0.25 to 0.25
Outputs:
- trunk_grad: float32 [1, 512, 512], replicated
- trunk_bias_grad: float32 [1, 512], replicated
- in_grad: float32 [4, 3, 4096], P('sx', None, 'sy')
- local_grad: float32 [4, 512, 4096], P('sx', None, 'sy')
- local_bias_grad: float32 [4, 4096], P('sx', 'sy')
- head_grad: float32 [4, 4096], P('sx', 'sy')
- loss_value: float32 [], replicated
The draws below stay inside these ranges and needn't reach their ends.
Inputs may be any that keep to these rules, and one draw needn't show every extreme that they name: `wall_index`: within a wall the positions are distinct. A shared wall has the same positions on both sides: wall 0 of (i, j) equals wall 1 of (i - 1, j), and wall 2 of (i, j) equals wall 3 of (i, (j - 1) mod 8).
All inputs are finite; a program needn't handle non-finite values.
Results may differ from the reference program's by a relative error of at most 0.0016.
Values sent between devices are 32-bit elements; how exact they have to be, the bound alone decides.
No kernel may reach another device: no remote copies, remote signals or barrier semaphores. Data moves between devices by JAX's collectives and lax.ppermute only.
A program may use at most 64 MiB of HBM per device.

```python
import jax
import jax.numpy as jnp
from jax import lax

W = 512
DEPTH = 1
PTS = 256
EDGE = 64
SLOTS = 1024
N_SX = 4
N_SY = 8


def draw_source(key, part):
    noise_field = jnp.clip(jax.random.normal(key, (N_SX, N_SY * PTS), jnp.float32), -4.0, 4.0)
    row_level = jnp.arange(N_SX, dtype=jnp.float32)[:, None]
    amplitude = 1.0 + 2.0 * row_level / max(N_SX - 1, 1)
    return amplitude * noise_field


def choose_slots(sub_key):
    return jax.random.permutation(sub_key, SLOTS)[:EDGE]


def draw_wall_index(key, part):
    x_keys = jax.random.split(jax.random.fold_in(key, 11), (N_SX + 1) * N_SY)
    y_keys = jax.random.split(jax.random.fold_in(key, 23), N_SX * N_SY)
    x_walls = jax.vmap(choose_slots)(x_keys).reshape(N_SX + 1, N_SY, EDGE)
    y_walls = jax.vmap(choose_slots)(y_keys).reshape(N_SX, N_SY, EDGE)
    west_side = x_walls[:-1]
    east_side = x_walls[1:]
    south_side = jnp.roll(y_walls, 1, axis=1)
    north_side = y_walls
    stacked = jnp.stack([west_side, east_side, south_side, north_side])
    return stacked.reshape(4, N_SX, N_SY * EDGE).astype(jnp.int32)


def with_ends(entries, own_key, low, top_value):
    longest = entries.shape.index(max(entries.shape))
    spots = []
    for shift in (0, 1):
        where = [jax.random.randint(jax.random.fold_in(own_key, axis), (), 0, length) for axis, length in enumerate(entries.shape)]
        where[longest] = (where[longest] + shift) % entries.shape[longest]
        spots.append(tuple(where))
    return entries.at[spots[0]].set(low).at[spots[1]].set(top_value)


def steps_of(key, dims, pieces, low, high):
    loudness, own = 1.0, jax.random.fold_in(key, 6)
    for position, shards_of in pieces:
        heights = jnp.exp(jax.random.uniform(jax.random.fold_in(own, position), (shards_of,), jnp.float32, low / len(pieces), high / len(pieces)))
        loudness = loudness * jnp.repeat(heights, dims[position] // shards_of).reshape([-1 if axis == position else 1 for axis in range(len(dims))])
    return loudness


def gaussian(key, shape, width, most, pieces=(), kind=jnp.bfloat16):
    level = steps_of(key, shape, pieces, -0.22, 0.18) if pieces else 1.0
    values = jax.random.normal(key, shape, jnp.float32) * width * level
    return jnp.minimum(jnp.maximum(values, -most), most).astype(kind)


def setup_inputs(seed: int = 0) -> dict:
    key_list = jax.random.split(jax.random.key(seed), 12)
    collocation = jnp.clip(jax.random.uniform(key_list[0], (2, N_SX, N_SY * PTS), jnp.float32, -1.0, 1.0) * steps_of(key_list[0], (2, N_SX, N_SY * PTS), ((1, 4), (2, 8)), -0.4, 0.0), -1.0, 1.0)
    source = draw_source(jax.random.fold_in(key_list[11], 71), 0)
    wall_index = draw_wall_index(jax.random.fold_in(key_list[11], 71), 0)
    bc_type = with_ends(jax.random.randint(key_list[3], (2, N_SY), 0, 2), jax.random.fold_in(key_list[3], 1), 0, 1).astype(jnp.int32)
    bc_value = gaussian(key_list[4], (2, N_SY * EDGE), 1.0, 4.0, ((1, 8),), jnp.float32)
    in_weight = gaussian(key_list[5], (N_SX, 3, N_SY * W), 2 ** -0.5, 4.0, ((0, 4), (2, 8)), jnp.float32)
    local_weight = gaussian(key_list[6], (N_SX, W, N_SY * W), W ** -0.5, 0.25, ((0, 4), (2, 8)))
    local_bias = gaussian(key_list[7], (N_SX, N_SY * W), 0.5, 3.0, ((0, 4), (1, 8)), jnp.float32)
    trunk_weight = gaussian(key_list[8], (DEPTH, W, W), W ** -0.5, 0.25)
    trunk_bias = gaussian(key_list[9], (DEPTH, W), 0.5, 3.0, (), jnp.float32)
    head_weight = gaussian(key_list[10], (N_SX, N_SY * W), W ** -0.5, 0.25, ((0, 4), (1, 8)), jnp.float32)
    return {"collocation": collocation, "source": source, "wall_index": wall_index, "bc_type": bc_type, "bc_value": bc_value, "in_weight": in_weight, "local_weight": local_weight, "local_bias": local_bias, "trunk_weight": trunk_weight, "trunk_bias": trunk_bias, "head_weight": head_weight}


HIGH = lax.Precision.HIGHEST
EPS = 1e-06

def activate(preact):
    values = jnp.tanh(preact[0])
    slopes = 1.0 - values * values
    result = [values, slopes * preact[1]]
    if preact.shape[0] == 5:
        curvature = -2.0 * values * slopes
        result.append(slopes * preact[2])
        result.append(slopes * preact[3] + curvature * preact[1] * preact[1])
        result.append(slopes * preact[4] + curvature * preact[2] * preact[2])
    return jnp.stack(result)

def entry_streams(coords, in_weight, directions):
    preact = coords[0][:, None] * in_weight[0] + coords[1][:, None] * in_weight[1] + in_weight[2]
    streams = [preact] + [jnp.broadcast_to(2.0 * in_weight[direction], preact.shape) for direction in directions]
    if len(directions) == 2:
        streams = streams + [jnp.zeros_like(preact), jnp.zeros_like(preact)]
    return jnp.stack(streams)

def layer_list(params):
    layers = [(params[1], params[2])]
    for layer_index in range(params[3].shape[0]):
        layers.append((params[3][layer_index], params[4][layer_index]))
    return layers

def run_forward(coords, directions, params):
    preact = entry_streams(coords, params[0], directions)
    activity, pullback = jax.vjp(activate, preact)
    pullbacks = [pullback]
    lowered = []
    for weight, layer_bias in layer_list(params):
        lowered_in = activity.astype(jnp.bfloat16)
        lowered.append(lowered_in)
        stream_count, row_count, breadth = lowered_in.shape
        product = jnp.dot(lowered_in.reshape(stream_count * row_count, breadth), weight, preferred_element_type=jnp.float32)
        preact = product.reshape(stream_count, row_count, -1)
        preact = preact.at[0].add(layer_bias)
        activity, pullback = jax.vjp(activate, preact)
        pullbacks.append(pullback)
    outputs = jnp.dot(activity, params[5], precision=HIGH)
    return (outputs, (activity, lowered, pullbacks))

def run_backward(coords, directions, params, tape, cotangent):
    activity, lowered, pullbacks = tape
    layers = layer_list(params)
    head_grad = jnp.einsum('kr,krw->w', cotangent, activity, precision=HIGH)
    upstream = cotangent[:, :, None] * params[5]
    weight_grads = []
    bias_grads = []
    for layer_index in reversed(range(len(layers))):
        preact_grad, = pullbacks[layer_index + 1](upstream)
        lowered_grad = preact_grad.astype(jnp.bfloat16)
        stream_count, row_count, breadth = lowered_grad.shape
        flat_grad = lowered_grad.reshape(stream_count * row_count, breadth)
        flat_input = lowered[layer_index].reshape(stream_count * row_count, -1)
        weight_grads.insert(0, lax.dot_general(flat_input, flat_grad, (((0,), (0,)), ((), ())), preferred_element_type=jnp.float32))
        bias_grads.insert(0, lax.optimization_barrier(jnp.sum(preact_grad[0], axis=0)))
        upstream = lax.dot_general(flat_grad, layers[layer_index][0], (((1,), (1,)), ((), ())), preferred_element_type=jnp.float32).reshape(stream_count, row_count, -1)
    entry_grad, = pullbacks[0](upstream)
    in_grad = jnp.concatenate([jnp.dot(coords, entry_grad[0], precision=HIGH), lax.optimization_barrier(jnp.sum(entry_grad[0], axis=0))[None]], axis=0)
    for stream, direction in enumerate(directions):
        in_grad = in_grad.at[direction].add(2.0 * lax.optimization_barrier(jnp.sum(entry_grad[1 + stream], axis=0)))
    return (in_grad, weight_grads[0], bias_grads[0], jnp.stack(weight_grads[1:]), jnp.stack(bias_grads[1:]), head_grad)

def wall_coords(wall_slots, slot_total):
    spots = (2.0 * wall_slots.astype(jnp.float32) + 1.0) / slot_total - 1.0
    unit_row = jnp.ones_like(spots[0])
    x_coords = jnp.stack([jnp.concatenate([-unit_row, unit_row]), jnp.concatenate([spots[0], spots[1]])])
    y_coords = jnp.stack([jnp.concatenate([spots[2], spots[3]]), jnp.concatenate([-unit_row, unit_row])])
    return (x_coords, y_coords)

def to_rims(outputs):
    half_size = outputs.shape[1] // 2
    return outputs.reshape(2, 2, half_size).transpose(1, 0, 2).reshape(2, 2 * half_size)

def residual_sum(outputs, forcing):
    residual = outputs[3] + outputs[4] + forcing
    return jnp.sum(residual * residual)

def wall_misfit(own_data, neighbour, target, bc_flag, is_outer, normal):
    half_size = own_data.shape[0] // 2
    interface = jnp.sum((own_data - neighbour) ** 2)
    dirichlet = jnp.sum((own_data[:half_size] - target) ** 2)
    neumann = jnp.sum((normal * own_data[half_size:] - target) ** 2)
    boundary = jnp.where(bc_flag == 0, dirichlet, neumann)
    return jnp.where(is_outer, boundary, interface)

def x_misfit(x_rims, neighbours, targets, bc_flags, at_start, at_end):
    return wall_misfit(x_rims[0], neighbours[0], targets[0], bc_flags[0], at_start, -1.0) + wall_misfit(x_rims[1], neighbours[1], targets[1], bc_flags[1], at_end, 1.0)

def y_misfit(y_rims, neighbours):
    return jnp.sum((y_rims - neighbours) ** 2)

def blend(inner_grads, wall_grads, inner_factor, wall_factor):
    return tuple((inner_factor * inner_part + wall_factor * wall_part for inner_part, wall_part in zip(inner_grads, wall_grads)))

def reference(collocation, source, wall_index, bc_type, bc_value, in_weight, local_weight, local_bias, trunk_weight, trunk_bias, head_weight):
    domain_total = N_SX * N_SY
    breadth = local_weight.shape[1]
    points_all = collocation.reshape(2, N_SX, N_SY, PTS).transpose(1, 2, 0, 3).reshape(domain_total, 2, PTS)
    forcing_all = source.reshape(domain_total, PTS)
    slots_all = wall_index.reshape(4, N_SX, N_SY, EDGE).transpose(1, 2, 0, 3).reshape(domain_total, 4, EDGE)
    entry_all = in_weight.reshape(N_SX, 3, N_SY, breadth).transpose(0, 2, 1, 3).reshape(domain_total, 3, breadth)
    own_all = local_weight.reshape(N_SX, breadth, N_SY, breadth).transpose(0, 2, 1, 3).reshape(domain_total, breadth, breadth)
    own_bias_all = local_bias.reshape(domain_total, breadth)
    head_all = head_weight.reshape(domain_total, breadth)
    targets_all = jnp.tile(bc_value.reshape(2, N_SY, EDGE).transpose(1, 0, 2), (N_SX, 1, 1))
    flags_all = jnp.tile(bc_type.T, (N_SX, 1))
    row_ids = jnp.repeat(jnp.arange(N_SX, dtype=jnp.int32), N_SY)

    def rims_of(item):
        wall_slots, entry_weight, own_weight, own_bias, own_head = item
        params = (entry_weight, own_weight, own_bias, trunk_weight, trunk_bias, own_head)
        x_coords, y_coords = wall_coords(wall_slots, SLOTS)
        x_out, x_tape = run_forward(x_coords, (0,), params)
        y_out, y_tape = run_forward(y_coords, (1,), params)
        return (to_rims(x_out), to_rims(y_out))
    x_all, y_all = lax.map(rims_of, (slots_all, entry_all, own_all, own_bias_all, head_all))
    x_grid = x_all.reshape(N_SX, N_SY, 2, 2 * EDGE)
    y_grid = y_all.reshape(N_SX, N_SY, 2, 2 * EDGE)
    blank = jnp.zeros((1, N_SY, 2 * EDGE), jnp.float32)
    west_side = jnp.concatenate([blank, x_grid[:-1, :, 1]], axis=0)
    east_side = jnp.concatenate([x_grid[1:, :, 0], blank], axis=0)
    south_side = jnp.roll(y_grid[:, :, 1], 1, axis=1)
    north_side = jnp.roll(y_grid[:, :, 0], -1, axis=1)
    x_near = jnp.stack([west_side, east_side], axis=2).reshape(domain_total, 2, 2 * EDGE)
    y_near = jnp.stack([south_side, north_side], axis=2).reshape(domain_total, 2, 2 * EDGE)

    def per_domain(running, item):
        points, forcing, wall_slots, entry_weight, own_weight, own_bias, own_head, x_nbr, y_nbr, targets, flags, row_id = item
        params = (entry_weight, own_weight, own_bias, trunk_weight, trunk_bias, own_head)
        x_coords, y_coords = wall_coords(wall_slots, SLOTS)
        x_out, x_tape = run_forward(x_coords, (0,), params)
        y_out, y_tape = run_forward(y_coords, (1,), params)
        inner_out, inner_tape = run_forward(points, (0, 1), params)
        residual_total, inner_cotangent = jax.value_and_grad(residual_sum)(inner_out, forcing)
        x_total, x_rim_grad = jax.value_and_grad(x_misfit)(to_rims(x_out), x_nbr, targets, flags, row_id == 0, row_id == N_SX - 1)
        y_total, y_rim_grad = jax.value_and_grad(y_misfit)(to_rims(y_out), y_nbr)
        inner_grads = run_backward(points, (0, 1), params, inner_tape, inner_cotangent)
        x_grads = run_backward(x_coords, (0,), params, x_tape, to_rims(x_rim_grad))
        y_grads = run_backward(y_coords, (1,), params, y_tape, to_rims(y_rim_grad))
        wall_grads = tuple((first_part + second_part for first_part, second_part in zip(x_grads, y_grads)))
        running = (running[0] + inner_grads[3], running[1] + inner_grads[4], running[2] + wall_grads[3], running[3] + wall_grads[4])
        emitted = (residual_total, x_total + y_total, inner_grads[0], inner_grads[1], inner_grads[2], inner_grads[5], wall_grads[0], wall_grads[1], wall_grads[2], wall_grads[5])
        return (running, emitted)
    start = (jnp.zeros(trunk_weight.shape, jnp.float32), jnp.zeros(trunk_bias.shape, jnp.float32), jnp.zeros(trunk_weight.shape, jnp.float32), jnp.zeros(trunk_bias.shape, jnp.float32))
    running, emitted = lax.scan(per_domain, start, (points_all, forcing_all, slots_all, entry_all, own_all, own_bias_all, head_all, x_near, y_near, targets_all, flags_all, row_ids))
    inner_count = PTS * domain_total
    wall_count = 4 * EDGE * domain_total
    inner_mean = jnp.sum(emitted[0]) / inner_count
    wall_mean = jnp.sum(emitted[1]) / wall_count
    balance_weight = jnp.sqrt((wall_mean + EPS) / (inner_mean + EPS))
    loss_value = balance_weight * inner_mean + wall_mean
    inner_factor = balance_weight / inner_count
    wall_factor = 1.0 / wall_count
    own_grads = blend(emitted[2:6], emitted[6:10], inner_factor, wall_factor)
    shared = blend((running[0], running[1]), (running[2], running[3]), inner_factor, wall_factor)
    in_grad = own_grads[0].reshape(N_SX, N_SY, 3, breadth).transpose(0, 2, 1, 3).reshape(N_SX, 3, N_SY * breadth)
    local_grad = own_grads[1].reshape(N_SX, N_SY, breadth, breadth).transpose(0, 2, 1, 3).reshape(N_SX, breadth, N_SY * breadth)
    local_bias_grad = own_grads[2].reshape(N_SX, N_SY * breadth)
    head_grad = own_grads[3].reshape(N_SX, N_SY * breadth)
    return (shared[0], shared[1], in_grad, local_grad, local_bias_grad, head_grad, loss_value)
```

```python
import functools

import jax
import jax.numpy as jnp
from jax import lax
from jax.experimental import pallas as pl
from jax.experimental.pallas import tpu as pltpu
from jax.sharding import PartitionSpec as P

SLOTS = 1024
EPS = 1e-06
TILE = 16
LANES = 128
F32 = jnp.float32
BF16 = jnp.bfloat16


def nn(a, b):
    return lax.dot_general(a, b, (((1,), (0,)), ((), ())), preferred_element_type=F32)


def nt(a, b):
    return lax.dot_general(a, b, (((1,), (1,)), ((), ())), preferred_element_type=F32)


def tn(a, b):
    return lax.dot_general(a, b, (((0,), (0,)), ((), ())), preferred_element_type=F32)


def eye_mask(rows, cols, shift=0):
    r = lax.broadcasted_iota(jnp.int32, (rows, cols), 0)
    c = lax.broadcasted_iota(jnp.int32, (rows, cols), 1)
    return r + shift == c


def to_column(row):
    size = row.shape[1]
    return jnp.sum(jnp.where(eye_mask(size, size), row, 0.0), axis=1, keepdims=True)


def chunks(width):
    return [slice(k, k + LANES) for k in range(0, width, LANES)]


def fold(parts):
    return [jnp.sum(p, axis=0, keepdims=True) for p in parts]


def zeros_tile():
    return jnp.zeros((TILE, LANES), F32)


def rows_of(i):
    return pl.ds(pl.multiple_of(i * TILE, TILE), TILE)


def wall_columns(index_ref, s_ref, t_ref):
    edge = index_ref.shape[2]
    shape = (edge, LANES)
    for w in range(4):
        spots = (2.0 * index_ref[w].astype(F32) + 1.0) / SLOTS - 1.0
        moving = jnp.broadcast_to(to_column(spots), shape)
        fixed = jnp.full(shape, -1.0 if w % 2 == 0 else 1.0, F32)
        where = pl.ds(w * edge, edge)
        s_ref[where, :] = fixed if w < 2 else moving
        t_ref[where, :] = moving if w < 2 else fixed


def wall_forward_kernel(*refs):
    far, refs = refs[:7], refs[7:]
    (rims_ref, s_ref, t_ref, a0_ref, x0_ref, z1_ref, x1_ref, z2_ref), refs = refs[:8], refs[8:]
    ua_ref, da_ref, sems = refs[:3]
    near = refs[3:]
    copies = [pltpu.make_async_copy(f, n, sems.at[k]) for k, (f, n) in enumerate(zip(far, near))]
    index_ref, win_ref, wl_ref, bl_ref, wt_ref, bt_ref, head_ref = near
    for copy in copies:
        copy.start()
    edge = index_ref.shape[2]
    points, width = a0_ref.shape
    copies[0].wait()
    copies[1].wait()
    wall_columns(index_ref, s_ref, t_ref)

    for direction in range(2):
        def entry(i, carry, direction=direction):
            rows = rows_of(i)
            s, t = s_ref[rows, :], t_ref[rows, :]
            for c in chunks(width):
                w0, w1, wb = (win_ref[k, :, c] for k in range(3))
                a = jnp.tanh(s * w0 + t * w1 + wb)
                slope = 1.0 - a * a
                a0_ref[rows, c] = a
                x0_ref[0, rows, c] = a.astype(BF16)
                x0_ref[1, rows, c] = (slope * (2.0 * (w0, w1)[direction])).astype(BF16)
            return carry

        tiles = points // (2 * TILE)
        lax.fori_loop(direction * tiles, (direction + 1) * tiles, entry, 0, unroll=2)

    for copy in copies[2:]:
        copy.wait()
    z1_ref[...] = nn(x0_ref[...].reshape(2 * points, width), wl_ref[0]).reshape(2, points, width)

    def hidden(i, carry):
        rows = rows_of(i)
        for c in chunks(width):
            a = jnp.tanh(z1_ref[0, rows, c] + bl_ref[:, c])
            slope = 1.0 - a * a
            z1_ref[0, rows, c] = a
            x1_ref[0, rows, c] = a.astype(BF16)
            x1_ref[1, rows, c] = (slope * z1_ref[1, rows, c]).astype(BF16)
        return carry

    lax.fori_loop(0, points // TILE, hidden, 0, unroll=2)
    z2_ref[...] = nn(x1_ref[...].reshape(2 * points, width), wt_ref[0]).reshape(2, points, width)

    def final(i, carry):
        rows = rows_of(i)
        u, d = zeros_tile(), zeros_tile()
        for c in chunks(width):
            a = jnp.tanh(z2_ref[0, rows, c] + bt_ref[:, c])
            slope = 1.0 - a * a
            z2_ref[0, rows, c] = a
            u += a * head_ref[:, c]
            d += slope * z2_ref[1, rows, c] * head_ref[:, c]
        ua_ref[rows, :] = u
        da_ref[rows, :] = d
        return carry

    lax.fori_loop(0, points // TILE, final, 0, unroll=2)
    value = jnp.sum(ua_ref[...], axis=1, keepdims=True)
    slope = jnp.sum(da_ref[...], axis=1, keepdims=True)
    low, high = eye_mask(edge, 2 * edge), eye_mask(edge, 2 * edge, edge)
    for w in range(4):
        part = slice(w * edge, (w + 1) * edge)
        both = jnp.where(low, value[part], 0.0) + jnp.where(high, slope[part], 0.0)
        rims_ref[w : w + 1, :] = jnp.sum(both, axis=0, keepdims=True)


def inner_kernel(
    order_size, order_of,
    points_ref, source_ref, win_ref, wl_ref, bl_ref, wt_ref, bt_ref, head_ref,
    grad_ref, sums_ref, s_ref, t_ref, a0_ref, x0_ref, z1_ref, g2_ref,
    x1_ref, z2_ref, acc_ref,
):
    points, width = a0_ref.shape
    for k in range(0, points, LANES):
        where = pl.ds(k, LANES)
        for ref, which in ((s_ref, 0), (t_ref, 1)):
            column = to_column(points_ref[which, :, k : k + LANES])
            ref[where, :] = jnp.broadcast_to(column, (LANES, LANES))

    def entry(i, carry):
        rows = rows_of(i)
        s, t = s_ref[rows, :], t_ref[rows, :]
        for c in chunks(width):
            w0, w1, wb = (win_ref[k, :, c] for k in range(3))
            p0, p1 = 2.0 * w0, 2.0 * w1
            a = jnp.tanh(s * w0 + t * w1 + wb)
            slope = 1.0 - a * a
            bend = -2.0 * a * slope
            a0_ref[rows, c] = a
            x0_ref[0, rows, c] = a.astype(BF16)
            x0_ref[1, rows, c] = (slope * p0).astype(BF16)
            x0_ref[2, rows, c] = (slope * p1).astype(BF16)
            x0_ref[3, rows, c] = (bend * (p0 * p0)).astype(BF16)
            x0_ref[4, rows, c] = (bend * (p1 * p1)).astype(BF16)
        return carry

    tiles = points // TILE
    lax.fori_loop(0, tiles, entry, 0, unroll=2)
    z1_ref[...] = nn(x0_ref[...].reshape(5 * points, width), wl_ref[0]).reshape(5, points, width)

    def hidden(i, carry):
        rows = rows_of(i)
        for c in chunks(width):
            a = jnp.tanh(z1_ref[0, rows, c] + bl_ref[:, c])
            p0, p1 = z1_ref[1, rows, c], z1_ref[2, rows, c]
            slope = 1.0 - a * a
            bend = -2.0 * a * slope
            z1_ref[0, rows, c] = a
            x1_ref[0, rows, c] = a.astype(BF16)
            x1_ref[1, rows, c] = (slope * p0).astype(BF16)
            x1_ref[2, rows, c] = (slope * p1).astype(BF16)
            x1_ref[3, rows, c] = (slope * z1_ref[3, rows, c] + bend * p0 * p0).astype(BF16)
            x1_ref[4, rows, c] = (slope * z1_ref[4, rows, c] + bend * p1 * p1).astype(BF16)
        return carry

    lax.fori_loop(0, tiles, hidden, 0, unroll=2)
    z2_ref[...] = nn(x1_ref[...].reshape(5 * points, width), wt_ref[0]).reshape(5, points, width)

    def final(i, carry):
        rows = rows_of(i)
        total = zeros_tile()
        for c in chunks(width):
            a = jnp.tanh(z2_ref[0, rows, c] + bt_ref[:, c])
            p0, p1 = z2_ref[1, rows, c], z2_ref[2, rows, c]
            slope = 1.0 - a * a
            bend = -2.0 * a * slope
            second = z2_ref[3, rows, c] + z2_ref[4, rows, c]
            bent = slope * second + bend * (p0 * p0 + p1 * p1)
            z2_ref[0, rows, c] = a
            z2_ref[3, rows, c] = second
            z2_ref[4, rows, c] = bent
            total += bent * head_ref[:, c]
        acc_ref[rows, :] = total
        return carry

    lax.fori_loop(0, tiles, final, 0, unroll=2)
    residual = jnp.sum(acc_ref[...], axis=1, keepdims=True)
    forcing = [to_column(source_ref[:, k : k + LANES]) for k in range(0, points, LANES)]
    residual = residual + jnp.concatenate(forcing, axis=0)
    acc_ref[...] = jnp.broadcast_to(2.0 * residual, acc_ref.shape)
    square = jnp.sum(residual * residual, axis=0, keepdims=True)

    spans = chunks(width)

    def top(i, carry):
        rows = rows_of(i)
        heads, biases = list(carry[0]), list(carry[1])
        twice = acc_ref[rows, :]
        for n, c in enumerate(spans):
            a = z2_ref[0, rows, c]
            p0, p1 = z2_ref[1, rows, c], z2_ref[2, rows, c]
            slope = 1.0 - a * a
            bend = -2.0 * a * slope
            g = twice * head_ref[:, c]
            heads[n] += twice * z2_ref[4, rows, c]
            gc = g * (p0 * p0 + p1 * p1)
            gs = g * z2_ref[3, rows, c] - 2.0 * a * gc
            g0 = slope * (-2.0 * (gc * slope + gs * a))
            bg = 2.0 * bend * g
            g3 = (slope * g).astype(BF16)
            biases[n] += g0
            g2_ref[0, rows, c] = g0.astype(BF16)
            g2_ref[1, rows, c] = (bg * p0).astype(BF16)
            g2_ref[2, rows, c] = (bg * p1).astype(BF16)
            g2_ref[3, rows, c] = g3
            g2_ref[4, rows, c] = g3
        return tuple(heads), tuple(biases)

    blank = tuple(zeros_tile() for _ in spans)
    heads, biases = lax.fori_loop(0, tiles, top, (blank, blank))
    sums_ref[...] = jnp.zeros(sums_ref.shape, F32)
    for c, hp, bp in zip(spans, fold(heads), fold(biases)):
        sums_ref[0:1, c] = bp
        sums_ref[1:2, c] = hp
    sums_ref[2:3, :] = jnp.broadcast_to(square, (1, width))
    store_ordered(
        grad_ref,
        tn(x1_ref[...].reshape(5 * points, width), g2_ref[...].reshape(5 * points, width)),
        order_size, order_of,
    )


def store_ordered(grad_ref, grad, order_size, order_of):
    mine, places = order_of
    size = grad.shape[0] // order_size
    mine = mine()
    for block in range(order_size):
        apart = mine ^ block
        place = 0
        for bit in places:
            place = place * 2 + ((apart >> bit) & 1)
        where = pl.ds(pl.multiple_of(place * size, size), size)
        grad_ref[where, :] = grad[block * size : (block + 1) * size]


def wall_top_kernel(
    order_size, order_of, row_size,
    rims_ref, west_ref, east_ref, south_ref, north_ref, type_ref, value_ref,
    z2_ref, x1_ref, head_ref, isums_ref,
    grad_ref, sums_ref, heads_ref, g2_ref,
    cu_ref, cd_ref,
):
    _, points, width = z2_ref.shape
    edge = points // 4
    place = lax.axis_index("sx")
    outer = (place == 0, place == row_size - 1)
    low, high = eye_mask(edge, 2 * edge), eye_mask(edge, 2 * edge, edge)
    total = jnp.zeros((1, 1), F32)

    def split(row):
        u = jnp.sum(jnp.where(low, row, 0.0), axis=1, keepdims=True)
        d = jnp.sum(jnp.where(high, row, 0.0), axis=1, keepdims=True)
        return u, d

    for w, near in enumerate((west_ref, east_ref, south_ref, north_ref)):
        u, d = split(rims_ref[w : w + 1, :])
        un, dn = split(near[...])
        eu, ed = u - un, d - dn
        if w < 2:
            normal = -1.0 if w == 0 else 1.0
            g = to_column(value_ref[w : w + 1, :])
            fixed = type_ref[:, w : w + 1] == 0
            bu = jnp.where(fixed, u - g, 0.0)
            bd = jnp.where(fixed, 0.0, normal * (normal * d - g))
            eu = jnp.where(outer[w], bu, eu)
            ed = jnp.where(outer[w], bd, ed)
        total += jnp.sum(eu * eu + ed * ed, axis=0, keepdims=True)
        where = pl.ds(w * edge, edge)
        cu_ref[where, :] = jnp.broadcast_to(2.0 * eu, (edge, LANES))
        cd_ref[where, :] = jnp.broadcast_to(2.0 * ed, (edge, LANES))

    spans = chunks(width)

    def top(i, carry):
        rows = rows_of(i)
        heads, biases = list(carry[0]), list(carry[1])
        cu, cd = cu_ref[rows, :], cd_ref[rows, :]
        for n, c in enumerate(spans):
            a, p = z2_ref[0, rows, c], z2_ref[1, rows, c]
            slope = 1.0 - a * a
            h = head_ref[:, c]
            gv, gd = cu * h, cd * h
            heads[n] += cu * a + cd * (slope * p)
            g0 = slope * (gv - 2.0 * a * (gd * p))
            biases[n] += g0
            g2_ref[0, rows, c] = g0.astype(BF16)
            g2_ref[1, rows, c] = (slope * gd).astype(BF16)
        return tuple(heads), tuple(biases)

    blank = tuple(zeros_tile() for _ in spans)
    heads, biases = lax.fori_loop(0, points // TILE, top, (blank, blank))
    sums_ref[...] = jnp.zeros(sums_ref.shape, F32)
    for c, hp, bp in zip(spans, fold(heads), fold(biases)):
        sums_ref[1:2, c] = bp
        heads_ref[:, c] = hp
    sums_ref[0:1, :] = isums_ref[0:1, :]
    sums_ref[2:3, :] = isums_ref[2:3, :]
    sums_ref[3:4, :] = jnp.broadcast_to(total, (1, width))
    store_ordered(
        grad_ref,
        tn(x1_ref[...].reshape(2 * points, width), g2_ref[...].reshape(2 * points, width)),
        order_size, order_of,
    )


def factors(total_r, total_b, inner_count, wall_count):
    mean_r = total_r / inner_count
    mean_b = total_b / wall_count
    lam = jnp.sqrt((mean_b + EPS) / (mean_r + EPS))
    return lam / inner_count, 1.0 / wall_count, lam * mean_r + mean_b


def unorder_kernel(order_size, order_of, *refs):
    ins, out_ref = refs[:order_size], refs[order_size]
    size = ins[0].shape[0]
    bits = order_size.bit_length() - 1
    mine = order_of()
    for place, ref in enumerate(ins):
        apart = sum(((place >> k) & 1) << (bits - 1 - k) for k in range(bits))
        where = pl.ds(pl.multiple_of((mine ^ apart) * size, size), size)
        out_ref[0, where, :] = ref[...]


def back(g_ref, count, weight, u_ref):
    _, size, width = g_ref.shape
    flat = g_ref[0:count].reshape(count * size, width)
    u_ref[...] = nt(flat, weight).reshape(count, size, width)


def hidden_kernel(
    wt_ref, z1i_ref, g2i_ref, z1w_ref, g2w_ref,
    gi_ref, gw_ref, biases_ref,
    ui_ref, uw_ref,
):
    _, points, width = z1i_ref.shape
    rims = z1w_ref.shape[1]
    spans = chunks(width)
    blank = tuple(zeros_tile() for _ in spans)

    back(g2i_ref, 4, wt_ref[0], ui_ref)

    def inner_hidden(i, carry):
        rows = rows_of(i)
        biases = list(carry)
        for n, c in enumerate(spans):
            a, p0, p1 = z1i_ref[0, rows, c], z1i_ref[1, rows, c], z1i_ref[2, rows, c]
            u0, u1, u2, u3 = (ui_ref[k, rows, c] for k in range(4))
            slope = 1.0 - a * a
            bend = -2.0 * a * slope
            gc = u3 * (p0 * p0 + p1 * p1)
            second = z1i_ref[3, rows, c] + z1i_ref[4, rows, c]
            gs = u1 * p0 + u2 * p1 + u3 * second - 2.0 * a * gc
            g0 = slope * (u0 - 2.0 * (gc * slope + gs * a))
            bg = 2.0 * bend * u3
            g3 = (slope * u3).astype(BF16)
            biases[n] += g0
            gi_ref[0, rows, c] = g0.astype(BF16)
            gi_ref[1, rows, c] = (slope * u1 + bg * p0).astype(BF16)
            gi_ref[2, rows, c] = (slope * u2 + bg * p1).astype(BF16)
            gi_ref[3, rows, c] = g3
            gi_ref[4, rows, c] = g3
        return tuple(biases)

    bias_i = lax.fori_loop(0, points // TILE, inner_hidden, blank)
    back(g2w_ref, 2, wt_ref[0], uw_ref)

    def wall_hidden(i, carry):
        rows = rows_of(i)
        biases = list(carry)
        for n, c in enumerate(spans):
            a, p = z1w_ref[0, rows, c], z1w_ref[1, rows, c]
            u0, u1 = uw_ref[0, rows, c], uw_ref[1, rows, c]
            slope = 1.0 - a * a
            g0 = slope * (u0 - 2.0 * a * (u1 * p))
            biases[n] += g0
            gw_ref[0, rows, c] = g0.astype(BF16)
            gw_ref[1, rows, c] = (slope * u1).astype(BF16)
        return tuple(biases)

    bias_w = lax.fori_loop(0, rims // TILE, wall_hidden, blank)
    biases_ref[...] = jnp.zeros(biases_ref.shape, F32)
    for c, bi, bw in zip(spans, fold(bias_i), fold(bias_w)):
        biases_ref[0:1, c] = bi
        biases_ref[1:2, c] = bw


def entry_kernel(
    win_ref, wl_ref,
    si_ref, ti_ref, a0i_ref, gi_ref, sw_ref, tw_ref, a0w_ref, gw_ref, biases_ref,
    parts_ref,
    ui_ref, uw_ref,
):
    points, width = a0i_ref.shape
    rims = a0w_ref.shape[0]
    spans = chunks(width)
    blank = tuple(zeros_tile() for _ in spans)
    back(gi_ref, 4, wl_ref[0], ui_ref)

    def inner_entry(i, carry):
        rows = rows_of(i)
        k0, k1, k2 = (list(part) for part in carry)
        s, t = si_ref[rows, :], ti_ref[rows, :]
        for n, c in enumerate(spans):
            a = a0i_ref[rows, c]
            p0, p1 = 2.0 * win_ref[0, :, c], 2.0 * win_ref[1, :, c]
            u0, u1, u2, u3 = (ui_ref[k, rows, c] for k in range(4))
            slope = 1.0 - a * a
            bend = -2.0 * a * slope
            gc = u3 * (p0 * p0 + p1 * p1)
            gs = u1 * p0 + u2 * p1 - 2.0 * a * gc
            g0 = slope * (u0 - 2.0 * (gc * slope + gs * a))
            bg = 2.0 * bend * u3
            k0[n] += s * g0 + 2.0 * (slope * u1 + bg * p0)
            k1[n] += t * g0 + 2.0 * (slope * u2 + bg * p1)
            k2[n] += g0
        return tuple(k0), tuple(k1), tuple(k2)

    entry_i = lax.fori_loop(0, points // TILE, inner_entry, (blank, blank, blank))
    back(gw_ref, 2, wl_ref[0], uw_ref)
    entry_w = (blank, blank, blank)
    for direction in range(2):
        def wall_entry(i, carry, direction=direction):
            rows = rows_of(i)
            k0, k1, k2 = (list(part) for part in carry)
            s, t = sw_ref[rows, :], tw_ref[rows, :]
            for n, c in enumerate(spans):
                a = a0w_ref[rows, c]
                p = 2.0 * win_ref[direction, :, c]
                u0, u1 = uw_ref[0, rows, c], uw_ref[1, rows, c]
                slope = 1.0 - a * a
                g0 = slope * (u0 - 2.0 * a * (u1 * p))
                along = 2.0 * (slope * u1)
                k0[n] += s * g0 + along if direction == 0 else s * g0
                k1[n] += t * g0 + along if direction == 1 else t * g0
                k2[n] += g0
            return tuple(k0), tuple(k1), tuple(k2)

        tiles = rims // (2 * TILE)
        entry_w = lax.fori_loop(direction * tiles, (direction + 1) * tiles, wall_entry, entry_w)
    parts_ref[3:4, :] = biases_ref[0:1, :]
    parts_ref[7:8, :] = biases_ref[1:2, :]
    for k in range(3):
        for c, ei, ew in zip(spans, fold(entry_i[k]), fold(entry_w[k])):
            parts_ref[k : k + 1, c] = ei
            parts_ref[4 + k : 5 + k, c] = ew


def blend_kernel(
    inner_count, wall_count,
    sums_ref, parts_ref, isums_ref, wheads_ref, x0i_ref, gi_ref, x0w_ref, gw_ref,
    in_ref, local_ref, bias_ref, head_ref, tbias_ref, loss_ref,
):
    count, points, width = x0i_ref.shape
    rims = x0w_ref.shape[1]
    fr, fb, loss = factors(sums_ref[2:3, :], sums_ref[3:4, :], inner_count, wall_count)
    loss_ref[...] = loss[:, 0:1]
    tbias_ref[...] = fr * sums_ref[0:1, :] + fb * sums_ref[1:2, :]
    head_ref[...] = fr * isums_ref[1:2, :] + fb * wheads_ref[...]
    for k in range(3):
        in_ref[k] = fr * parts_ref[k : k + 1, :] + fb * parts_ref[4 + k : 5 + k, :]
    bias_ref[...] = fr * parts_ref[3:4, :] + fb * parts_ref[7:8, :]
    local_ref[0] = fr * tn(
        x0i_ref[...].reshape(count * points, width), gi_ref[...].reshape(count * points, width)
    ) + fb * tn(x0w_ref[...].reshape(2 * rims, width), gw_ref[...].reshape(2 * rims, width))


def call(kernel, outs, scratch, args, flops, name, space=pltpu.VMEM):
    vmem = pl.BlockSpec(memory_space=pltpu.VMEM)
    return pl.pallas_call(
        kernel,
        out_shape=outs,
        in_specs=[pl.BlockSpec(memory_space=space)] * len(args),
        out_specs=jax.tree.map(lambda _: vmem, outs),
        scratch_shapes=scratch,
        compiler_params=pltpu.CompilerParams(vmem_limit_bytes=20 << 20),
        cost_estimate=pl.CostEstimate(flops=flops, bytes_accessed=0, transcendentals=0),
        name=name,
    )(*args)


def shape(*dims, dtype=F32):
    return jax.ShapeDtypeStruct(dims, dtype)


def swap(x, axis, bit):
    size = lax.axis_size(axis)
    return lax.ppermute(x, axis, [(i, i ^ (1 << bit)) for i in range(size)])


def bits_of(axis):
    return [(axis, bit) for bit in range(lax.axis_size(axis).bit_length() - 1)]


def neighbours(lower, upper, axis, wrap):
    size = lax.axis_size(axis)
    even = lax.axis_index(axis) % 2 == 0
    within, across = [], []
    for i in range(0, size, 2):
        within += [(i, i + 1), (i + 1, i)]
        if wrap or i + 2 < size:
            across += [(i + 1, (i + 2) % size), ((i + 2) % size, i + 1)]
    far = lax.ppermute(jnp.where(even, lower, upper), axis, across)
    close = lax.ppermute(jnp.where(even, upper, lower), axis, within)
    return jnp.where(even, far, close), jnp.where(even, close, far)


def together(*xs):
    return lax.optimization_barrier(xs)


def per_device(
    collocation, source, wall_index, bc_type, bc_value,
    in_weight, local_weight, local_bias, trunk_weight, trunk_bias, head_weight,
):
    rows, cols = lax.axis_size("sx"), lax.axis_size("sy")
    assert rows & (rows - 1) == 0 and cols & (cols - 1) == 0 and rows >= 4 and cols >= 2
    points, edge, width = collocation.shape[2], wall_index.shape[2], local_weight.shape[1]
    rims_total = 4 * edge
    inner_count = float(points * rows * cols)
    wall_count = float(rims_total * rows * cols)

    core, first, second = ("sy", 0), ("sx", 0), ("sx", 1)
    halved = (core, first, second)
    doubled = [b for b in bits_of("sy") + bits_of("sx") if b not in halved]
    order_size = 1 << len(halved)

    def mine():
        return sum(((lax.axis_index(axis) >> bit) & 1) << k for k, (axis, bit) in enumerate(halved))

    order_r, order_b = (mine, (0, 1, 2)), (mine, (0, 2, 1))

    big = shape(width, width)
    small = shape(8, width)

    def stack(count, size, dtype=F32):
        return shape(count, size, width, dtype=dtype)

    def vm(s):
        return pltpu.VMEM(s.shape, s.dtype)

    entry_weight = jnp.transpose(in_weight, (1, 0, 2))
    firsts = (wall_index, entry_weight, local_weight, local_bias, trunk_weight, trunk_bias, head_weight)
    (rims, sw, tw, a0w, x0w, z1w, x1w, z2w) = call(
        wall_forward_kernel,
        (
            shape(4, 2 * edge), shape(rims_total, LANES), shape(rims_total, LANES),
            shape(rims_total, width), stack(2, rims_total, BF16), stack(2, rims_total),
            stack(2, rims_total, BF16), stack(2, rims_total),
        ),
        [pltpu.VMEM((rims_total, LANES), F32)] * 2
        + [pltpu.SemaphoreType.DMA((len(firsts),))]
        + [vm(x) for x in firsts],
        tuple(pltpu.with_memory_space_constraint(x, pltpu.HBM) for x in firsts),
        4 * rims_total * 2 * width * width,
        "wall_forward",
        pltpu.HBM,
    )
    south, north = neighbours(rims[2:3], rims[3:4], "sy", True)
    west, east = neighbours(rims[0:1], rims[1:2], "sx", False)

    (grad_r, isums, si, ti, a0i, x0i, z1i, g2i) = call(
        functools.partial(inner_kernel, order_size, order_r),
        (
            big, small, shape(points, LANES), shape(points, LANES), shape(points, width),
            stack(5, points, BF16), stack(5, points), stack(5, points, BF16),
        ),
        [vm(stack(5, points, BF16)), vm(stack(5, points)), pltpu.VMEM((points, LANES), F32)],
        (collocation, source, entry_weight, local_weight, local_bias, trunk_weight, trunk_bias, head_weight),
        6 * points * 5 * width * width,
        "inner",
    )
    (grad_b, sums, wheads, g2w) = call(
        functools.partial(wall_top_kernel, order_size, order_b, rows),
        (big, small, shape(1, width), stack(2, rims_total, BF16)),
        [pltpu.VMEM((rims_total, LANES), F32)] * 2,
        (rims, west, east, south, north, bc_type.T, bc_value, z2w, x1w, head_weight, isums),
        2 * rims_total * 2 * width * width,
        "wall_top",
    )
    half = width // 2
    got_r = swap(grad_r[half:], *core)
    sums = sums + swap(sums, *core)
    got_b = swap(grad_b[half:], *core)
    quarter = half // 2
    send_r, keep_r = grad_r[quarter:half] + got_r[quarter:], grad_r[:quarter] + got_r[:quarter]
    send_b, keep_b = grad_b[quarter:half] + got_b[quarter:], grad_b[:quarter] + got_b[:quarter]
    sums, send_r = together(sums, send_r)
    more = swap(sums, *first)
    got_r = swap(send_r, *first)
    got_b = swap(send_b, *second)
    sums = sums + more
    eighth = quarter // 2
    send_r, keep_r = keep_r[eighth:] + got_r[eighth:], keep_r[:eighth] + got_r[:eighth]
    send_b, keep_b = keep_b[eighth:] + got_b[eighth:], keep_b[:eighth] + got_b[:eighth]
    for axis, bit in doubled:
        sums = sums + swap(sums, axis, bit)
    sums, send_r = together(sums, send_r)
    got_b = swap(send_b, *first)
    more = swap(sums, *second)
    got_r = swap(send_r, *second)
    sums = sums + more
    fr, fb, _ = factors(sums[2:3], sums[3:4], inner_count, wall_count)
    block = fr * (keep_r + got_r) + fb * (keep_b + got_b)
    block, g2w = together(block, g2w)
    gi, gw, biases = call(
        hidden_kernel,
        (stack(5, points, BF16), stack(2, rims_total, BF16), small),
        [vm(stack(4, points)), vm(stack(2, rims_total))],
        (trunk_weight, z1i, g2i, z1w, g2w),
        2 * (points * 4 + rims_total * 2) * width * width,
        "hidden",
    )
    for axis, bit in doubled[:-1]:
        block = block + swap(block, axis, bit)
    block, biases = together(block, biases)
    parts = call(
        entry_kernel,
        small,
        [vm(stack(4, points)), vm(stack(2, rims_total))],
        (entry_weight, local_weight, si, ti, a0i, gi, sw, tw, a0w, gw, biases),
        2 * (points * 4 + rims_total * 2) * width * width,
        "entry",
    )
    for axis, bit in doubled[-1:]:
        block = block + swap(block, axis, bit)
    block, parts = together(block, parts)
    in_grad, local_grad, local_bias_grad, head_grad, trunk_bias_grad, loss = call(
        functools.partial(blend_kernel, inner_count, wall_count),
        (shape(3, 1, width), shape(1, width, width)) + (shape(1, width),) * 3 + (shape(1, 1),),
        [],
        (sums, parts, isums, wheads, x0i, gi, x0w, gw),
        2 * (points * 5 + rims_total * 2) * width * width,
        "blend",
    )
    blocks = [block, swap(block, *second)]
    blocks = blocks + [swap(b, *first) for b in blocks]
    *blocks, local_bias_grad = together(*blocks, local_bias_grad)
    blocks = blocks + [swap(b, *core) for b in blocks]
    trunk_grad = call(
        functools.partial(unorder_kernel, order_size, mine),
        shape(1, width, width),
        [],
        tuple(blocks),
        width * width,
        "unorder",
    )
    return (
        trunk_grad, trunk_bias_grad, jnp.transpose(in_grad, (1, 0, 2)), local_grad,
        local_bias_grad, head_grad, loss.reshape(()),
    )


def solution(mesh):
    return jax.shard_map(
        per_device,
        mesh=mesh,
        in_specs=(
            P(None, "sx", "sy"),
            P("sx", "sy"),
            P(None, "sx", "sy"),
            P(None, "sy"),
            P(None, "sy"),
            P("sx", None, "sy"),
            P("sx", None, "sy"),
            P("sx", "sy"),
            P(),
            P(),
            P("sx", "sy"),
        ),
        out_specs=(
            P(),
            P(),
            P("sx", None, "sy"),
            P("sx", None, "sy"),
            P("sx", "sy"),
            P("sx", "sy"),
            P(),
        ),
        check_vma=False,
    )
```

```python
import functools

import jax
import jax.numpy as jnp
from jax import lax
from jax.experimental import pallas as pl
from jax.experimental.pallas import tpu as pltpu
from jax.sharding import PartitionSpec as P


SLOTS = 1024
EPS = 1e-06
TILE = 16
LANES = 128
F32 = jnp.float32
BF16 = jnp.bfloat16


def nn(a, b):
    return lax.dot_general(a, b, (((1,), (0,)), ((), ())), preferred_element_type=F32)


def nt(a, b):
    return lax.dot_general(a, b, (((1,), (1,)), ((), ())), preferred_element_type=F32)


def tn(a, b):
    return lax.dot_general(a, b, (((0,), (0,)), ((), ())), preferred_element_type=F32)


def eye_mask(rows, cols, shift=0):
    r = lax.broadcasted_iota(jnp.int32, (rows, cols), 0)
    c = lax.broadcasted_iota(jnp.int32, (rows, cols), 1)
    return r + shift == c


def to_column(row):
    size = row.shape[1]
    return jnp.sum(jnp.where(eye_mask(size, size), row, 0.0), axis=1, keepdims=True)


def chunks(width):
    return [slice(k, k + LANES) for k in range(0, width, LANES)]


def fold(parts):
    return [jnp.sum(p, axis=0, keepdims=True) for p in parts]


def zeros_tile():
    return jnp.zeros((TILE, LANES), F32)


def rows_of(i):
    return pl.ds(pl.multiple_of(i * TILE, TILE), TILE)


def wall_columns(index_ref, s_ref, t_ref):
    edge = index_ref.shape[2]
    shape = (edge, LANES)
    for w in range(4):
        spots = (2.0 * index_ref[w].astype(F32) + 1.0) / SLOTS - 1.0
        moving = jnp.broadcast_to(to_column(spots), shape)
        fixed = jnp.full(shape, -1.0 if w % 2 == 0 else 1.0, F32)
        where = pl.ds(w * edge, edge)
        s_ref[where, :] = fixed if w < 2 else moving
        t_ref[where, :] = moving if w < 2 else fixed


def wall_forward_kernel(*refs):
    far, refs = refs[:7], refs[7:]
    (rims_ref, s_ref, t_ref, a0_ref, x0_ref, z1_ref, x1_ref, z2_ref), refs = refs[:8], refs[8:]
    ua_ref, da_ref, sems = refs[:3]
    near = refs[3:]
    copies = [pltpu.make_async_copy(f, n, sems.at[k]) for k, (f, n) in enumerate(zip(far, near))]
    index_ref, win_ref, wl_ref, bl_ref, wt_ref, bt_ref, head_ref = near
    for copy in copies:
        copy.start()
    edge = index_ref.shape[2]
    points, width = a0_ref.shape
    copies[0].wait()
    copies[1].wait()
    wall_columns(index_ref, s_ref, t_ref)

    for direction in range(2):
        def entry(i, carry, direction=direction):
            rows = rows_of(i)
            s, t = s_ref[rows, :], t_ref[rows, :]
            for c in chunks(width):
                w0, w1, wb = (win_ref[k, :, c] for k in range(3))
                a = jnp.tanh(s * w0 + t * w1 + wb)
                slope = 1.0 - a * a
                a0_ref[rows, c] = a
                x0_ref[0, rows, c] = a.astype(BF16)
                x0_ref[1, rows, c] = (slope * (2.0 * (w0, w1)[direction])).astype(BF16)
            return carry

        tiles = points // (2 * TILE)
        lax.fori_loop(direction * tiles, (direction + 1) * tiles, entry, 0, unroll=2)

    for copy in copies[2:]:
        copy.wait()
    z1_ref[...] = nn(x0_ref[...].reshape(2 * points, width), wl_ref[0]).reshape(2, points, width)

    def hidden(i, carry):
        rows = rows_of(i)
        for c in chunks(width):
            a = jnp.tanh(z1_ref[0, rows, c] + bl_ref[:, c])
            slope = 1.0 - a * a
            z1_ref[0, rows, c] = a
            x1_ref[0, rows, c] = a.astype(BF16)
            x1_ref[1, rows, c] = (slope * z1_ref[1, rows, c]).astype(BF16)
        return carry

    lax.fori_loop(0, points // TILE, hidden, 0, unroll=2)
    z2_ref[...] = nn(x1_ref[...].reshape(2 * points, width), wt_ref[0]).reshape(2, points, width)

    def final(i, carry):
        rows = rows_of(i)
        u, d = zeros_tile(), zeros_tile()
        for c in chunks(width):
            a = jnp.tanh(z2_ref[0, rows, c] + bt_ref[:, c])
            slope = 1.0 - a * a
            z2_ref[0, rows, c] = a
            u += a * head_ref[:, c]
            d += slope * z2_ref[1, rows, c] * head_ref[:, c]
        ua_ref[rows, :] = u
        da_ref[rows, :] = d
        return carry

    lax.fori_loop(0, points // TILE, final, 0, unroll=2)
    value = jnp.sum(ua_ref[...], axis=1, keepdims=True)
    slope = jnp.sum(da_ref[...], axis=1, keepdims=True)
    low, high = eye_mask(edge, 2 * edge), eye_mask(edge, 2 * edge, edge)
    for w in range(4):
        part = slice(w * edge, (w + 1) * edge)
        both = jnp.where(low, value[part], 0.0) + jnp.where(high, slope[part], 0.0)
        rims_ref[w : w + 1, :] = jnp.sum(both, axis=0, keepdims=True)


def inner_kernel(
    order_size, order_of,
    points_ref, source_ref, win_ref, wl_ref, bl_ref, wt_ref, bt_ref, head_ref,
    grad_ref, sums_ref, s_ref, t_ref, a0_ref, x0_ref, z1_ref, g2_ref,
    x1_ref, z2_ref, acc_ref,
):
    points, width = a0_ref.shape
    for k in range(0, points, LANES):
        where = pl.ds(k, LANES)
        for ref, which in ((s_ref, 0), (t_ref, 1)):
            column = to_column(points_ref[which, :, k : k + LANES])
            ref[where, :] = jnp.broadcast_to(column, (LANES, LANES))

    def entry(i, carry):
        rows = rows_of(i)
        s, t = s_ref[rows, :], t_ref[rows, :]
        for c in chunks(width):
            w0, w1, wb = (win_ref[k, :, c] for k in range(3))
            p0, p1 = 2.0 * w0, 2.0 * w1
            a = jnp.tanh(s * w0 + t * w1 + wb)
            slope = 1.0 - a * a
            bend = -2.0 * a * slope
            a0_ref[rows, c] = a
            x0_ref[0, rows, c] = a.astype(BF16)
            x0_ref[1, rows, c] = (slope * p0).astype(BF16)
            x0_ref[2, rows, c] = (slope * p1).astype(BF16)
            x0_ref[3, rows, c] = (bend * (p0 * p0)).astype(BF16)
            x0_ref[4, rows, c] = (bend * (p1 * p1)).astype(BF16)
        return carry

    tiles = points // TILE
    lax.fori_loop(0, tiles, entry, 0, unroll=2)
    z1_ref[...] = nn(x0_ref[...].reshape(5 * points, width), wl_ref[0]).reshape(5, points, width)

    def hidden(i, carry):
        rows = rows_of(i)
        for c in chunks(width):
            a = jnp.tanh(z1_ref[0, rows, c] + bl_ref[:, c])
            p0, p1 = z1_ref[1, rows, c], z1_ref[2, rows, c]
            slope = 1.0 - a * a
            bend = -2.0 * a * slope
            z1_ref[0, rows, c] = a
            x1_ref[0, rows, c] = a.astype(BF16)
            x1_ref[1, rows, c] = (slope * p0).astype(BF16)
            x1_ref[2, rows, c] = (slope * p1).astype(BF16)
            x1_ref[3, rows, c] = (slope * z1_ref[3, rows, c] + bend * p0 * p0).astype(BF16)
            x1_ref[4, rows, c] = (slope * z1_ref[4, rows, c] + bend * p1 * p1).astype(BF16)
        return carry

    lax.fori_loop(0, tiles, hidden, 0, unroll=2)
    z2_ref[...] = nn(x1_ref[...].reshape(5 * points, width), wt_ref[0]).reshape(5, points, width)

    def final(i, carry):
        rows = rows_of(i)
        total = zeros_tile()
        for c in chunks(width):
            a = jnp.tanh(z2_ref[0, rows, c] + bt_ref[:, c])
            p0, p1 = z2_ref[1, rows, c], z2_ref[2, rows, c]
            slope = 1.0 - a * a
            bend = -2.0 * a * slope
            second = z2_ref[3, rows, c] + z2_ref[4, rows, c]
            bent = slope * second + bend * (p0 * p0 + p1 * p1)
            z2_ref[0, rows, c] = a
            z2_ref[3, rows, c] = second
            z2_ref[4, rows, c] = bent
            total += bent * head_ref[:, c]
        acc_ref[rows, :] = total
        return carry

    lax.fori_loop(0, tiles, final, 0, unroll=2)
    residual = jnp.sum(acc_ref[...], axis=1, keepdims=True)
    forcing = [to_column(source_ref[:, k : k + LANES]) for k in range(0, points, LANES)]
    residual = residual + jnp.concatenate(forcing, axis=0)
    acc_ref[...] = jnp.broadcast_to(2.0 * residual, acc_ref.shape)
    square = jnp.sum(residual * residual, axis=0, keepdims=True)

    spans = chunks(width)

    def top(i, carry):
        rows = rows_of(i)
        heads, biases = list(carry[0]), list(carry[1])
        twice = acc_ref[rows, :]
        for n, c in enumerate(spans):
            a = z2_ref[0, rows, c]
            p0, p1 = z2_ref[1, rows, c], z2_ref[2, rows, c]
            slope = 1.0 - a * a
            bend = -2.0 * a * slope
            g = twice * head_ref[:, c]
            heads[n] += twice * z2_ref[4, rows, c]
            gc = g * (p0 * p0 + p1 * p1)
            gs = g * z2_ref[3, rows, c] - 2.0 * a * gc
            g0 = slope * (-2.0 * (gc * slope + gs * a))
            bg = 2.0 * bend * g
            g3 = (slope * g).astype(BF16)
            biases[n] += g0
            g2_ref[0, rows, c] = g0.astype(BF16)
            g2_ref[1, rows, c] = (bg * p0).astype(BF16)
            g2_ref[2, rows, c] = (bg * p1).astype(BF16)
            g2_ref[3, rows, c] = g3
            g2_ref[4, rows, c] = g3
        return tuple(heads), tuple(biases)

    blank = tuple(zeros_tile() for _ in spans)
    heads, biases = lax.fori_loop(0, tiles, top, (blank, blank))
    sums_ref[...] = jnp.zeros(sums_ref.shape, F32)
    for c, hp, bp in zip(spans, fold(heads), fold(biases)):
        sums_ref[0:1, c] = bp
        sums_ref[1:2, c] = hp
    sums_ref[2:3, :] = jnp.broadcast_to(square, (1, width))
    store_ordered(
        grad_ref,
        tn(x1_ref[...].reshape(5 * points, width), g2_ref[...].reshape(5 * points, width)),
        order_size, order_of,
    )


def store_ordered(grad_ref, grad, order_size, order_of):
    mine = order_of()
    size = grad.shape[0] // order_size
    for block in range(order_size):
        where = pl.ds(pl.multiple_of((mine ^ block) * size, size), size)
        grad_ref[where, :] = grad[block * size : (block + 1) * size]


def wall_top_kernel(
    order_size, order_of, row_size,
    rims_ref, west_ref, east_ref, south_ref, north_ref, type_ref, value_ref,
    z2_ref, x1_ref, head_ref, isums_ref,
    grad_ref, sums_ref, heads_ref, g2_ref,
    cu_ref, cd_ref,
):
    _, points, width = z2_ref.shape
    edge = points // 4
    place = lax.axis_index("sx")
    outer = (place == 0, place == row_size - 1)
    low, high = eye_mask(edge, 2 * edge), eye_mask(edge, 2 * edge, edge)
    total = jnp.zeros((1, 1), F32)

    def split(row):
        u = jnp.sum(jnp.where(low, row, 0.0), axis=1, keepdims=True)
        d = jnp.sum(jnp.where(high, row, 0.0), axis=1, keepdims=True)
        return u, d

    for w, near in enumerate((west_ref, east_ref, south_ref, north_ref)):
        u, d = split(rims_ref[w : w + 1, :])
        un, dn = split(near[...])
        eu, ed = u - un, d - dn
        if w < 2:
            normal = -1.0 if w == 0 else 1.0
            g = to_column(value_ref[w : w + 1, :])
            fixed = type_ref[:, w : w + 1] == 0
            bu = jnp.where(fixed, u - g, 0.0)
            bd = jnp.where(fixed, 0.0, normal * (normal * d - g))
            eu = jnp.where(outer[w], bu, eu)
            ed = jnp.where(outer[w], bd, ed)
        total += jnp.sum(eu * eu + ed * ed, axis=0, keepdims=True)
        where = pl.ds(w * edge, edge)
        cu_ref[where, :] = jnp.broadcast_to(2.0 * eu, (edge, LANES))
        cd_ref[where, :] = jnp.broadcast_to(2.0 * ed, (edge, LANES))

    spans = chunks(width)

    def top(i, carry):
        rows = rows_of(i)
        heads, biases = list(carry[0]), list(carry[1])
        cu, cd = cu_ref[rows, :], cd_ref[rows, :]
        for n, c in enumerate(spans):
            a, p = z2_ref[0, rows, c], z2_ref[1, rows, c]
            slope = 1.0 - a * a
            h = head_ref[:, c]
            gv, gd = cu * h, cd * h
            heads[n] += cu * a + cd * (slope * p)
            g0 = slope * (gv - 2.0 * a * (gd * p))
            biases[n] += g0
            g2_ref[0, rows, c] = g0.astype(BF16)
            g2_ref[1, rows, c] = (slope * gd).astype(BF16)
        return tuple(heads), tuple(biases)

    blank = tuple(zeros_tile() for _ in spans)
    heads, biases = lax.fori_loop(0, points // TILE, top, (blank, blank))
    sums_ref[...] = jnp.zeros(sums_ref.shape, F32)
    for c, hp, bp in zip(spans, fold(heads), fold(biases)):
        sums_ref[1:2, c] = bp
        heads_ref[:, c] = hp
    sums_ref[0:1, :] = isums_ref[0:1, :]
    sums_ref[2:3, :] = isums_ref[2:3, :]
    sums_ref[3:4, :] = jnp.broadcast_to(total, (1, width))
    store_ordered(
        grad_ref,
        tn(x1_ref[...].reshape(2 * points, width), g2_ref[...].reshape(2 * points, width)),
        order_size, order_of,
    )


def factors(total_r, total_b, inner_count, wall_count):
    mean_r = total_r / inner_count
    mean_b = total_b / wall_count
    lam = jnp.sqrt((mean_b + EPS) / (mean_r + EPS))
    return lam / inner_count, 1.0 / wall_count, lam * mean_r + mean_b


def unorder_kernel(order_size, order_of, *refs):
    ins, out_ref = refs[:order_size], refs[order_size]
    size = ins[0].shape[0]
    mine = order_of()
    for place, ref in enumerate(ins):
        where = pl.ds(pl.multiple_of((mine ^ place) * size, size), size)
        out_ref[0, where, :] = ref[...]


def back(g_ref, count, weight, u_ref):
    _, size, width = g_ref.shape
    flat = g_ref[0:count].reshape(count * size, width)
    u_ref[...] = nt(flat, weight).reshape(count, size, width)


def hidden_kernel(
    wt_ref, z1i_ref, g2i_ref, z1w_ref, g2w_ref,
    gi_ref, gw_ref, biases_ref,
    ui_ref, uw_ref,
):
    _, points, width = z1i_ref.shape
    rims = z1w_ref.shape[1]
    spans = chunks(width)
    blank = tuple(zeros_tile() for _ in spans)

    back(g2i_ref, 4, wt_ref[0], ui_ref)

    def inner_hidden(i, carry):
        rows = rows_of(i)
        biases = list(carry)
        for n, c in enumerate(spans):
            a, p0, p1 = z1i_ref[0, rows, c], z1i_ref[1, rows, c], z1i_ref[2, rows, c]
            u0, u1, u2, u3 = (ui_ref[k, rows, c] for k in range(4))
            slope = 1.0 - a * a
            bend = -2.0 * a * slope
            gc = u3 * (p0 * p0 + p1 * p1)
            second = z1i_ref[3, rows, c] + z1i_ref[4, rows, c]
            gs = u1 * p0 + u2 * p1 + u3 * second - 2.0 * a * gc
            g0 = slope * (u0 - 2.0 * (gc * slope + gs * a))
            bg = 2.0 * bend * u3
            g3 = (slope * u3).astype(BF16)
            biases[n] += g0
            gi_ref[0, rows, c] = g0.astype(BF16)
            gi_ref[1, rows, c] = (slope * u1 + bg * p0).astype(BF16)
            gi_ref[2, rows, c] = (slope * u2 + bg * p1).astype(BF16)
            gi_ref[3, rows, c] = g3
            gi_ref[4, rows, c] = g3
        return tuple(biases)

    bias_i = lax.fori_loop(0, points // TILE, inner_hidden, blank)
    back(g2w_ref, 2, wt_ref[0], uw_ref)

    def wall_hidden(i, carry):
        rows = rows_of(i)
        biases = list(carry)
        for n, c in enumerate(spans):
            a, p = z1w_ref[0, rows, c], z1w_ref[1, rows, c]
            u0, u1 = uw_ref[0, rows, c], uw_ref[1, rows, c]
            slope = 1.0 - a * a
            g0 = slope * (u0 - 2.0 * a * (u1 * p))
            biases[n] += g0
            gw_ref[0, rows, c] = g0.astype(BF16)
            gw_ref[1, rows, c] = (slope * u1).astype(BF16)
        return tuple(biases)

    bias_w = lax.fori_loop(0, rims // TILE, wall_hidden, blank)
    biases_ref[...] = jnp.zeros(biases_ref.shape, F32)
    for c, bi, bw in zip(spans, fold(bias_i), fold(bias_w)):
        biases_ref[0:1, c] = bi
        biases_ref[1:2, c] = bw


def entry_kernel(
    win_ref, wl_ref,
    si_ref, ti_ref, a0i_ref, gi_ref, sw_ref, tw_ref, a0w_ref, gw_ref, biases_ref,
    parts_ref,
    ui_ref, uw_ref,
):
    points, width = a0i_ref.shape
    rims = a0w_ref.shape[0]
    spans = chunks(width)
    blank = tuple(zeros_tile() for _ in spans)
    back(gi_ref, 4, wl_ref[0], ui_ref)

    def inner_entry(i, carry):
        rows = rows_of(i)
        k0, k1, k2 = (list(part) for part in carry)
        s, t = si_ref[rows, :], ti_ref[rows, :]
        for n, c in enumerate(spans):
            a = a0i_ref[rows, c]
            p0, p1 = 2.0 * win_ref[0, :, c], 2.0 * win_ref[1, :, c]
            u0, u1, u2, u3 = (ui_ref[k, rows, c] for k in range(4))
            slope = 1.0 - a * a
            bend = -2.0 * a * slope
            gc = u3 * (p0 * p0 + p1 * p1)
            gs = u1 * p0 + u2 * p1 - 2.0 * a * gc
            g0 = slope * (u0 - 2.0 * (gc * slope + gs * a))
            bg = 2.0 * bend * u3
            k0[n] += s * g0 + 2.0 * (slope * u1 + bg * p0)
            k1[n] += t * g0 + 2.0 * (slope * u2 + bg * p1)
            k2[n] += g0
        return tuple(k0), tuple(k1), tuple(k2)

    entry_i = lax.fori_loop(0, points // TILE, inner_entry, (blank, blank, blank))
    back(gw_ref, 2, wl_ref[0], uw_ref)
    entry_w = (blank, blank, blank)
    for direction in range(2):
        def wall_entry(i, carry, direction=direction):
            rows = rows_of(i)
            k0, k1, k2 = (list(part) for part in carry)
            s, t = sw_ref[rows, :], tw_ref[rows, :]
            for n, c in enumerate(spans):
                a = a0w_ref[rows, c]
                p = 2.0 * win_ref[direction, :, c]
                u0, u1 = uw_ref[0, rows, c], uw_ref[1, rows, c]
                slope = 1.0 - a * a
                g0 = slope * (u0 - 2.0 * a * (u1 * p))
                along = 2.0 * (slope * u1)
                k0[n] += s * g0 + along if direction == 0 else s * g0
                k1[n] += t * g0 + along if direction == 1 else t * g0
                k2[n] += g0
            return tuple(k0), tuple(k1), tuple(k2)

        tiles = rims // (2 * TILE)
        entry_w = lax.fori_loop(direction * tiles, (direction + 1) * tiles, wall_entry, entry_w)
    parts_ref[3:4, :] = biases_ref[0:1, :]
    parts_ref[7:8, :] = biases_ref[1:2, :]
    for k in range(3):
        for c, ei, ew in zip(spans, fold(entry_i[k]), fold(entry_w[k])):
            parts_ref[k : k + 1, c] = ei
            parts_ref[4 + k : 5 + k, c] = ew


def blend_kernel(
    inner_count, wall_count,
    sums_ref, parts_ref, isums_ref, wheads_ref, x0i_ref, gi_ref, x0w_ref, gw_ref,
    in_ref, local_ref, bias_ref, head_ref, tbias_ref, loss_ref,
):
    count, points, width = x0i_ref.shape
    rims = x0w_ref.shape[1]
    fr, fb, loss = factors(sums_ref[2:3, :], sums_ref[3:4, :], inner_count, wall_count)
    loss_ref[...] = loss[:, 0:1]
    tbias_ref[...] = fr * sums_ref[0:1, :] + fb * sums_ref[1:2, :]
    head_ref[...] = fr * isums_ref[1:2, :] + fb * wheads_ref[...]
    for k in range(3):
        in_ref[k] = fr * parts_ref[k : k + 1, :] + fb * parts_ref[4 + k : 5 + k, :]
    bias_ref[...] = fr * parts_ref[3:4, :] + fb * parts_ref[7:8, :]
    local_ref[0] = fr * tn(
        x0i_ref[...].reshape(count * points, width), gi_ref[...].reshape(count * points, width)
    ) + fb * tn(x0w_ref[...].reshape(2 * rims, width), gw_ref[...].reshape(2 * rims, width))


def call(kernel, outs, scratch, args, flops, space=pltpu.VMEM):
    vmem = pl.BlockSpec(memory_space=pltpu.VMEM)
    return pl.pallas_call(
        kernel,
        out_shape=outs,
        in_specs=[pl.BlockSpec(memory_space=space)] * len(args),
        out_specs=jax.tree.map(lambda _: vmem, outs),
        scratch_shapes=scratch,
        compiler_params=pltpu.CompilerParams(vmem_limit_bytes=20 << 20),
        cost_estimate=pl.CostEstimate(flops=flops, bytes_accessed=0, transcendentals=0),
    )(*args)


def shape(*dims, dtype=F32):
    return jax.ShapeDtypeStruct(dims, dtype)


def swap(x, axis, bit):
    return exchange(x, axis, 1 << bit)


def exchange(x, axis, mask):
    return lax.ppermute(x, axis, [(i, i ^ mask) for i in range(lax.axis_size(axis))])


def bits_of(axis):
    return [(axis, bit) for bit in range(lax.axis_size(axis).bit_length() - 1)]


def neighbours(lower, upper, axis):
    size = lax.axis_size(axis)
    even = lax.axis_index(axis) % 2 == 0
    within, across = [], []
    for i in range(0, size, 2):
        within += [(i, i + 1), (i + 1, i)]
        across += [(i + 1, (i + 2) % size), ((i + 2) % size, i + 1)]
    far = lax.ppermute(jnp.where(even, lower, upper), axis, across)
    close = lax.ppermute(jnp.where(even, upper, lower), axis, within)
    return jnp.where(even, far, close), jnp.where(even, close, far)


def together(*xs):
    return lax.optimization_barrier(xs)


def per_device(
    collocation, source, wall_index, bc_type, bc_value,
    in_weight, local_weight, local_bias, trunk_weight, trunk_bias, head_weight,
):
    rows, cols = lax.axis_size("sx"), lax.axis_size("sy")
    assert rows & (rows - 1) == 0 and cols & (cols - 1) == 0 and rows >= 4 and cols >= 2
    points, edge, width = collocation.shape[2], wall_index.shape[2], local_weight.shape[1]
    rims_total = 4 * edge
    inner_count = float(points * rows * cols)
    wall_count = float(rims_total * rows * cols)

    core = ("sy", 0)
    halved = (("sx", 0), ("sx", 1), core)
    doubled = [b for b in bits_of("sy") + bits_of("sx") if b not in halved]
    order_size = 1 << len(halved)

    def mine():
        return sum(((lax.axis_index(axis) >> bit) & 1) << k for k, (axis, bit) in enumerate(halved))

    big = shape(width, width)
    small = shape(8, width)

    def stack(count, size, dtype=F32):
        return shape(count, size, width, dtype=dtype)

    def vm(s):
        return pltpu.VMEM(s.shape, s.dtype)

    entry_weight = jnp.transpose(in_weight, (1, 0, 2))
    firsts = (wall_index, entry_weight, local_weight, local_bias, trunk_weight, trunk_bias, head_weight)
    (rims, sw, tw, a0w, x0w, z1w, x1w, z2w) = call(
        wall_forward_kernel,
        (
            shape(4, 2 * edge), shape(rims_total, LANES), shape(rims_total, LANES),
            shape(rims_total, width), stack(2, rims_total, BF16), stack(2, rims_total),
            stack(2, rims_total, BF16), stack(2, rims_total),
        ),
        [pltpu.VMEM((rims_total, LANES), F32)] * 2
        + [pltpu.SemaphoreType.DMA((len(firsts),))]
        + [vm(x) for x in firsts],
        tuple(pltpu.with_memory_space_constraint(x, pltpu.HBM) for x in firsts),
        4 * rims_total * 2 * width * width,
        pltpu.HBM,
    )
    south, north = neighbours(rims[2:3], rims[3:4], "sy")
    west, east = neighbours(rims[0:1], rims[1:2], "sx")

    (grad_r, isums, si, ti, a0i, x0i, z1i, g2i) = call(
        functools.partial(inner_kernel, order_size, mine),
        (
            big, small, shape(points, LANES), shape(points, LANES), shape(points, width),
            stack(5, points, BF16), stack(5, points), stack(5, points, BF16),
        ),
        [vm(stack(5, points, BF16)), vm(stack(5, points)), pltpu.VMEM((points, LANES), F32)],
        (collocation, source, entry_weight, local_weight, local_bias, trunk_weight, trunk_bias, head_weight),
        6 * points * 5 * width * width,
    )
    (grad_b, sums, wheads, g2w) = call(
        functools.partial(wall_top_kernel, order_size, mine, rows),
        (big, small, shape(1, width), stack(2, rims_total, BF16)),
        [pltpu.VMEM((rims_total, LANES), F32)] * 2,
        (rims, west, east, south, north, bc_type.T, bc_value, z2w, x1w, head_weight, isums),
        2 * rims_total * 2 * width * width,
    )
    half = width // 2
    got_r = swap(grad_r[half:], *core)
    grad_r = grad_r[:half] + got_r
    more = swap(sums, *core)
    sums = sums + more
    got_b = swap(grad_b[half:], *core)
    grad_b = grad_b[:half] + got_b
    part = half // 4
    gots = []
    for mask in (1, 2, 3):
        where = slice(mask * part, (mask + 1) * part)
        trio = []
        for x in (sums, grad_r[where], grad_b[where]):
            trio.append(exchange(x, "sx", mask))
        gots.append(trio)
    sums = sums + gots[0][0] + gots[1][0] + gots[2][0]
    keep_r = grad_r[:part] + gots[0][1] + gots[1][1] + gots[2][1]
    keep_b = grad_b[:part] + gots[0][2] + gots[1][2] + gots[2][2]
    sums, g2w = together(sums, g2w)
    for axis, bit in doubled:
        more = swap(sums, axis, bit)
        sums = sums + more
    gi, gw, biases = call(
        hidden_kernel,
        (stack(5, points, BF16), stack(2, rims_total, BF16), small),
        [vm(stack(4, points)), vm(stack(2, rims_total))],
        (trunk_weight, z1i, g2i, z1w, g2w),
        2 * (points * 4 + rims_total * 2) * width * width,
    )
    fr, fb, _ = factors(sums[2:3], sums[3:4], inner_count, wall_count)
    block = fr * keep_r + fb * keep_b
    block, biases = together(block, biases)
    for axis, bit in doubled[:1]:
        block = block + swap(block, axis, bit)
    parts = call(
        entry_kernel,
        small,
        [vm(stack(4, points)), vm(stack(2, rims_total))],
        (entry_weight, local_weight, si, ti, a0i, gi, sw, tw, a0w, gw, biases),
        2 * (points * 4 + rims_total * 2) * width * width,
    )
    block, parts = together(block, parts)
    for axis, bit in doubled[1:]:
        block = block + swap(block, axis, bit)
    in_grad, local_grad, local_bias_grad, head_grad, trunk_bias_grad, loss = call(
        functools.partial(blend_kernel, inner_count, wall_count),
        (shape(3, 1, width), shape(1, width, width)) + (shape(1, width),) * 3 + (shape(1, 1),),
        [],
        (sums, parts, isums, wheads, x0i, gi, x0w, gw),
        2 * (points * 5 + rims_total * 2) * width * width,
    )
    blocks = [block]
    for mask in (1, 2, 3):
        blocks.append(exchange(block, "sx", mask))
    *blocks, local_bias_grad = together(*blocks, local_bias_grad)
    blocks = blocks + [swap(b, *core) for b in blocks]
    trunk_grad = call(
        functools.partial(unorder_kernel, order_size, mine),
        shape(1, width, width),
        [],
        tuple(blocks),
        width * width,
    )
    return (
        trunk_grad, trunk_bias_grad, jnp.transpose(in_grad, (1, 0, 2)), local_grad,
        local_bias_grad, head_grad, loss.reshape(()),
    )


def solution(mesh):
    return jax.shard_map(
        per_device,
        mesh=mesh,
        in_specs=(
            P(None, "sx", "sy"),
            P("sx", "sy"),
            P(None, "sx", "sy"),
            P(None, "sy"),
            P(None, "sy"),
            P("sx", None, "sy"),
            P("sx", None, "sy"),
            P("sx", "sy"),
            P(),
            P(),
            P("sx", "sy"),
        ),
        out_specs=(
            P(),
            P(),
            P("sx", None, "sy"),
            P("sx", None, "sy"),
            P("sx", "sy"),
            P("sx", "sy"),
            P(),
        ),
        check_vma=False,
    )
```

```python
import functools

import jax
import jax.numpy as jnp
from jax import lax
from jax.experimental import pallas as pl
from jax.experimental.pallas import tpu as pltpu
from jax.sharding import PartitionSpec as P


SLOTS = 1024
EPS = 1e-06
TILE = 16
LANES = 128
F32 = jnp.float32
BF16 = jnp.bfloat16


def nn(a, b):
    return lax.dot_general(a, b, (((1,), (0,)), ((), ())), preferred_element_type=F32)


def nt(a, b):
    return lax.dot_general(a, b, (((1,), (1,)), ((), ())), preferred_element_type=F32)


def tn(a, b):
    return lax.dot_general(a, b, (((0,), (0,)), ((), ())), preferred_element_type=F32)


def eye_mask(rows, cols, shift=0):
    r = lax.broadcasted_iota(jnp.int32, (rows, cols), 0)
    c = lax.broadcasted_iota(jnp.int32, (rows, cols), 1)
    return r + shift == c


def to_column(row):
    size = row.shape[1]
    return jnp.sum(jnp.where(eye_mask(size, size), row, 0.0), axis=1, keepdims=True)


def chunks(width):
    return [slice(k, k + LANES) for k in range(0, width, LANES)]


def fold(parts):
    return [jnp.sum(p, axis=0, keepdims=True) for p in parts]


def zeros_tile():
    return jnp.zeros((TILE, LANES), F32)


def rows_of(i):
    return pl.ds(pl.multiple_of(i * TILE, TILE), TILE)


def wall_columns(index_ref, s_ref, t_ref):
    edge = index_ref.shape[2]
    shape = (edge, LANES)
    for w in range(4):
        spots = (2.0 * index_ref[w].astype(F32) + 1.0) / SLOTS - 1.0
        moving = jnp.broadcast_to(to_column(spots), shape)
        fixed = jnp.full(shape, -1.0 if w % 2 == 0 else 1.0, F32)
        where = pl.ds(w * edge, edge)
        s_ref[where, :] = fixed if w < 2 else moving
        t_ref[where, :] = moving if w < 2 else fixed


def wall_forward_kernel(*refs):
    far, refs = refs[:7], refs[7:]
    (rims_ref, s_ref, t_ref, a0_ref, x0_ref, z1_ref, x1_ref, z2_ref), refs = refs[:8], refs[8:]
    ua_ref, da_ref, sems = refs[:3]
    near = refs[3:]
    copies = [pltpu.make_async_copy(f, n, sems.at[k]) for k, (f, n) in enumerate(zip(far, near))]
    index_ref, win_ref, wl_ref, bl_ref, wt_ref, bt_ref, head_ref = near
    for copy in copies:
        copy.start()
    edge = index_ref.shape[2]
    points, width = a0_ref.shape
    copies[0].wait()
    copies[1].wait()
    wall_columns(index_ref, s_ref, t_ref)

    for direction in range(2):
        def entry(i, carry, direction=direction):
            rows = rows_of(i)
            s, t = s_ref[rows, :], t_ref[rows, :]
            for c in chunks(width):
                w0, w1, wb = (win_ref[k, :, c] for k in range(3))
                a = jnp.tanh(s * w0 + t * w1 + wb)
                slope = 1.0 - a * a
                a0_ref[rows, c] = a
                x0_ref[0, rows, c] = a.astype(BF16)
                x0_ref[1, rows, c] = (slope * (2.0 * (w0, w1)[direction])).astype(BF16)
            return carry

        tiles = points // (2 * TILE)
        lax.fori_loop(direction * tiles, (direction + 1) * tiles, entry, 0, unroll=2)

    for copy in copies[2:]:
        copy.wait()
    z1_ref[...] = nn(x0_ref[...].reshape(2 * points, width), wl_ref[0]).reshape(2, points, width)

    def hidden(i, carry):
        rows = rows_of(i)
        for c in chunks(width):
            a = jnp.tanh(z1_ref[0, rows, c] + bl_ref[:, c])
            slope = 1.0 - a * a
            z1_ref[0, rows, c] = a
            x1_ref[0, rows, c] = a.astype(BF16)
            x1_ref[1, rows, c] = (slope * z1_ref[1, rows, c]).astype(BF16)
        return carry

    lax.fori_loop(0, points // TILE, hidden, 0, unroll=2)
    z2_ref[...] = nn(x1_ref[...].reshape(2 * points, width), wt_ref[0]).reshape(2, points, width)

    def final(i, carry):
        rows = rows_of(i)
        u, d = zeros_tile(), zeros_tile()
        for c in chunks(width):
            a = jnp.tanh(z2_ref[0, rows, c] + bt_ref[:, c])
            slope = 1.0 - a * a
            z2_ref[0, rows, c] = a
            u += a * head_ref[:, c]
            d += slope * z2_ref[1, rows, c] * head_ref[:, c]
        ua_ref[rows, :] = u
        da_ref[rows, :] = d
        return carry

    lax.fori_loop(0, points // TILE, final, 0, unroll=2)
    value = jnp.sum(ua_ref[...], axis=1, keepdims=True)
    slope = jnp.sum(da_ref[...], axis=1, keepdims=True)
    low, high = eye_mask(edge, 2 * edge), eye_mask(edge, 2 * edge, edge)
    for w in range(4):
        part = slice(w * edge, (w + 1) * edge)
        both = jnp.where(low, value[part], 0.0) + jnp.where(high, slope[part], 0.0)
        rims_ref[w : w + 1, :] = jnp.sum(both, axis=0, keepdims=True)


def inner_kernel(
    order_size, order_of,
    points_ref, source_ref, win_ref, wl_ref, bl_ref, wt_ref, bt_ref, head_ref,
    grad_ref, sums_ref, s_ref, t_ref, a0_ref, x0_ref, z1_ref, g2_ref,
    x1_ref, z2_ref, acc_ref,
):
    points, width = a0_ref.shape
    for k in range(0, points, LANES):
        where = pl.ds(k, LANES)
        for ref, which in ((s_ref, 0), (t_ref, 1)):
            column = to_column(points_ref[which, :, k : k + LANES])
            ref[where, :] = jnp.broadcast_to(column, (LANES, LANES))

    def entry(i, carry):
        rows = rows_of(i)
        s, t = s_ref[rows, :], t_ref[rows, :]
        for c in chunks(width):
            w0, w1, wb = (win_ref[k, :, c] for k in range(3))
            p0, p1 = 2.0 * w0, 2.0 * w1
            a = jnp.tanh(s * w0 + t * w1 + wb)
            slope = 1.0 - a * a
            bend = -2.0 * a * slope
            a0_ref[rows, c] = a
            x0_ref[0, rows, c] = a.astype(BF16)
            x0_ref[1, rows, c] = (slope * p0).astype(BF16)
            x0_ref[2, rows, c] = (slope * p1).astype(BF16)
            x0_ref[3, rows, c] = (bend * (p0 * p0)).astype(BF16)
            x0_ref[4, rows, c] = (bend * (p1 * p1)).astype(BF16)
        return carry

    tiles = points // TILE
    lax.fori_loop(0, tiles, entry, 0, unroll=2)
    z1_ref[...] = nn(x0_ref[...].reshape(5 * points, width), wl_ref[0]).reshape(5, points, width)

    def hidden(i, carry):
        rows = rows_of(i)
        for c in chunks(width):
            a = jnp.tanh(z1_ref[0, rows, c] + bl_ref[:, c])
            p0, p1 = z1_ref[1, rows, c], z1_ref[2, rows, c]
            slope = 1.0 - a * a
            bend = -2.0 * a * slope
            z1_ref[0, rows, c] = a
            x1_ref[0, rows, c] = a.astype(BF16)
            x1_ref[1, rows, c] = (slope * p0).astype(BF16)
            x1_ref[2, rows, c] = (slope * p1).astype(BF16)
            x1_ref[3, rows, c] = (slope * z1_ref[3, rows, c] + bend * p0 * p0).astype(BF16)
            x1_ref[4, rows, c] = (slope * z1_ref[4, rows, c] + bend * p1 * p1).astype(BF16)
        return carry

    lax.fori_loop(0, tiles, hidden, 0, unroll=2)
    z2_ref[...] = nn(x1_ref[...].reshape(5 * points, width), wt_ref[0]).reshape(5, points, width)

    def final(i, carry):
        rows = rows_of(i)
        total = zeros_tile()
        for c in chunks(width):
            a = jnp.tanh(z2_ref[0, rows, c] + bt_ref[:, c])
            p0, p1 = z2_ref[1, rows, c], z2_ref[2, rows, c]
            slope = 1.0 - a * a
            bend = -2.0 * a * slope
            second = z2_ref[3, rows, c] + z2_ref[4, rows, c]
            bent = slope * second + bend * (p0 * p0 + p1 * p1)
            z2_ref[0, rows, c] = a
            z2_ref[3, rows, c] = second
            z2_ref[4, rows, c] = bent
            total += bent * head_ref[:, c]
        acc_ref[rows, :] = total
        return carry

    lax.fori_loop(0, tiles, final, 0, unroll=2)
    residual = jnp.sum(acc_ref[...], axis=1, keepdims=True)
    forcing = [to_column(source_ref[:, k : k + LANES]) for k in range(0, points, LANES)]
    residual = residual + jnp.concatenate(forcing, axis=0)
    acc_ref[...] = jnp.broadcast_to(2.0 * residual, acc_ref.shape)
    square = jnp.sum(residual * residual, axis=0, keepdims=True)

    spans = chunks(width)

    def top(i, carry):
        rows = rows_of(i)
        heads, biases = list(carry[0]), list(carry[1])
        twice = acc_ref[rows, :]
        for n, c in enumerate(spans):
            a = z2_ref[0, rows, c]
            p0, p1 = z2_ref[1, rows, c], z2_ref[2, rows, c]
            slope = 1.0 - a * a
            bend = -2.0 * a * slope
            g = twice * head_ref[:, c]
            heads[n] += twice * z2_ref[4, rows, c]
            gc = g * (p0 * p0 + p1 * p1)
            gs = g * z2_ref[3, rows, c] - 2.0 * a * gc
            g0 = slope * (-2.0 * (gc * slope + gs * a))
            bg = 2.0 * bend * g
            g3 = (slope * g).astype(BF16)
            biases[n] += g0
            g2_ref[0, rows, c] = g0.astype(BF16)
            g2_ref[1, rows, c] = (bg * p0).astype(BF16)
            g2_ref[2, rows, c] = (bg * p1).astype(BF16)
            g2_ref[3, rows, c] = g3
            g2_ref[4, rows, c] = g3
        return tuple(heads), tuple(biases)

    blank = tuple(zeros_tile() for _ in spans)
    heads, biases = lax.fori_loop(0, tiles, top, (blank, blank))
    sums_ref[...] = jnp.zeros(sums_ref.shape, F32)
    for c, hp, bp in zip(spans, fold(heads), fold(biases)):
        sums_ref[0:1, c] = bp
        sums_ref[1:2, c] = hp
    sums_ref[2:3, :] = jnp.broadcast_to(square, (1, width))
    store_ordered(
        grad_ref,
        tn(x1_ref[...].reshape(5 * points, width), g2_ref[...].reshape(5 * points, width)),
        order_size, order_of,
    )


def store_ordered(grad_ref, grad, order_size, order_of):
    mine = order_of()
    size = grad.shape[0] // order_size
    for block in range(order_size):
        where = pl.ds(pl.multiple_of((mine ^ block) * size, size), size)
        grad_ref[where, :] = grad[block * size : (block + 1) * size]


def wall_top_kernel(
    order_size, order_of, row_size,
    rims_ref, west_ref, east_ref, south_ref, north_ref, type_ref, value_ref,
    z2_ref, x1_ref, head_ref, isums_ref,
    grad_ref, sums_ref, heads_ref, g2_ref,
    cu_ref, cd_ref,
):
    _, points, width = z2_ref.shape
    edge = points // 4
    place = lax.axis_index("sx")
    outer = (place == 0, place == row_size - 1)
    low, high = eye_mask(edge, 2 * edge), eye_mask(edge, 2 * edge, edge)
    total = jnp.zeros((1, 1), F32)

    def split(row):
        u = jnp.sum(jnp.where(low, row, 0.0), axis=1, keepdims=True)
        d = jnp.sum(jnp.where(high, row, 0.0), axis=1, keepdims=True)
        return u, d

    for w, near in enumerate((west_ref, east_ref, south_ref, north_ref)):
        u, d = split(rims_ref[w : w + 1, :])
        un, dn = split(near[...])
        eu, ed = u - un, d - dn
        if w < 2:
            normal = -1.0 if w == 0 else 1.0
            g = to_column(value_ref[w : w + 1, :])
            fixed = type_ref[:, w : w + 1] == 0
            bu = jnp.where(fixed, u - g, 0.0)
            bd = jnp.where(fixed, 0.0, normal * (normal * d - g))
            eu = jnp.where(outer[w], bu, eu)
            ed = jnp.where(outer[w], bd, ed)
        total += jnp.sum(eu * eu + ed * ed, axis=0, keepdims=True)
        where = pl.ds(w * edge, edge)
        cu_ref[where, :] = jnp.broadcast_to(2.0 * eu, (edge, LANES))
        cd_ref[where, :] = jnp.broadcast_to(2.0 * ed, (edge, LANES))

    spans = chunks(width)

    def top(i, carry):
        rows = rows_of(i)
        heads, biases = list(carry[0]), list(carry[1])
        cu, cd = cu_ref[rows, :], cd_ref[rows, :]
        for n, c in enumerate(spans):
            a, p = z2_ref[0, rows, c], z2_ref[1, rows, c]
            slope = 1.0 - a * a
            h = head_ref[:, c]
            gv, gd = cu * h, cd * h
            heads[n] += cu * a + cd * (slope * p)
            g0 = slope * (gv - 2.0 * a * (gd * p))
            biases[n] += g0
            g2_ref[0, rows, c] = g0.astype(BF16)
            g2_ref[1, rows, c] = (slope * gd).astype(BF16)
        return tuple(heads), tuple(biases)

    blank = tuple(zeros_tile() for _ in spans)
    heads, biases = lax.fori_loop(0, points // TILE, top, (blank, blank))
    sums_ref[...] = jnp.zeros(sums_ref.shape, F32)
    for c, hp, bp in zip(spans, fold(heads), fold(biases)):
        sums_ref[1:2, c] = bp
        heads_ref[:, c] = hp
    sums_ref[0:1, :] = isums_ref[0:1, :]
    sums_ref[2:3, :] = isums_ref[2:3, :]
    sums_ref[3:4, :] = jnp.broadcast_to(total, (1, width))
    store_ordered(
        grad_ref,
        tn(x1_ref[...].reshape(2 * points, width), g2_ref[...].reshape(2 * points, width)),
        order_size, order_of,
    )


def factors(total_r, total_b, inner_count, wall_count):
    mean_r = total_r / inner_count
    mean_b = total_b / wall_count
    lam = jnp.sqrt((mean_b + EPS) / (mean_r + EPS))
    return lam / inner_count, 1.0 / wall_count, lam * mean_r + mean_b


def unorder_kernel(order_size, order_of, *refs):
    ins, out_ref = refs[:order_size], refs[order_size]
    size = ins[0].shape[0]
    mine = order_of()
    for place, ref in enumerate(ins):
        where = pl.ds(pl.multiple_of((mine ^ place) * size, size), size)
        out_ref[0, where, :] = ref[...]


def back(g_ref, count, weight, u_ref):
    _, size, width = g_ref.shape
    flat = g_ref[0:count].reshape(count * size, width)
    u_ref[...] = nt(flat, weight).reshape(count, size, width)


def hidden_kernel(
    wt_ref, z1i_ref, g2i_ref, z1w_ref, g2w_ref,
    gi_ref, gw_ref, biases_ref,
    ui_ref, uw_ref,
):
    _, points, width = z1i_ref.shape
    rims = z1w_ref.shape[1]
    spans = chunks(width)
    blank = tuple(zeros_tile() for _ in spans)

    back(g2i_ref, 4, wt_ref[0], ui_ref)

    def inner_hidden(i, carry):
        rows = rows_of(i)
        biases = list(carry)
        for n, c in enumerate(spans):
            a, p0, p1 = z1i_ref[0, rows, c], z1i_ref[1, rows, c], z1i_ref[2, rows, c]
            u0, u1, u2, u3 = (ui_ref[k, rows, c] for k in range(4))
            slope = 1.0 - a * a
            bend = -2.0 * a * slope
            gc = u3 * (p0 * p0 + p1 * p1)
            second = z1i_ref[3, rows, c] + z1i_ref[4, rows, c]
            gs = u1 * p0 + u2 * p1 + u3 * second - 2.0 * a * gc
            g0 = slope * (u0 - 2.0 * (gc * slope + gs * a))
            bg = 2.0 * bend * u3
            g3 = (slope * u3).astype(BF16)
            biases[n] += g0
            gi_ref[0, rows, c] = g0.astype(BF16)
            gi_ref[1, rows, c] = (slope * u1 + bg * p0).astype(BF16)
            gi_ref[2, rows, c] = (slope * u2 + bg * p1).astype(BF16)
            gi_ref[3, rows, c] = g3
            gi_ref[4, rows, c] = g3
        return tuple(biases)

    bias_i = lax.fori_loop(0, points // TILE, inner_hidden, blank)
    back(g2w_ref, 2, wt_ref[0], uw_ref)

    def wall_hidden(i, carry):
        rows = rows_of(i)
        biases = list(carry)
        for n, c in enumerate(spans):
            a, p = z1w_ref[0, rows, c], z1w_ref[1, rows, c]
            u0, u1 = uw_ref[0, rows, c], uw_ref[1, rows, c]
            slope = 1.0 - a * a
            g0 = slope * (u0 - 2.0 * a * (u1 * p))
            biases[n] += g0
            gw_ref[0, rows, c] = g0.astype(BF16)
            gw_ref[1, rows, c] = (slope * u1).astype(BF16)
        return tuple(biases)

    bias_w = lax.fori_loop(0, rims // TILE, wall_hidden, blank)
    biases_ref[...] = jnp.zeros(biases_ref.shape, F32)
    for c, bi, bw in zip(spans, fold(bias_i), fold(bias_w)):
        biases_ref[0:1, c] = bi
        biases_ref[1:2, c] = bw


def entry_kernel(
    win_ref, wl_ref,
    si_ref, ti_ref, a0i_ref, gi_ref, sw_ref, tw_ref, a0w_ref, gw_ref, biases_ref,
    parts_ref,
    ui_ref, uw_ref,
):
    points, width = a0i_ref.shape
    rims = a0w_ref.shape[0]
    spans = chunks(width)
    blank = tuple(zeros_tile() for _ in spans)
    back(gi_ref, 4, wl_ref[0], ui_ref)

    def inner_entry(i, carry):
        rows = rows_of(i)
        k0, k1, k2 = (list(part) for part in carry)
        s, t = si_ref[rows, :], ti_ref[rows, :]
        for n, c in enumerate(spans):
            a = a0i_ref[rows, c]
            p0, p1 = 2.0 * win_ref[0, :, c], 2.0 * win_ref[1, :, c]
            u0, u1, u2, u3 = (ui_ref[k, rows, c] for k in range(4))
            slope = 1.0 - a * a
            bend = -2.0 * a * slope
            gc = u3 * (p0 * p0 + p1 * p1)
            gs = u1 * p0 + u2 * p1 - 2.0 * a * gc
            g0 = slope * (u0 - 2.0 * (gc * slope + gs * a))
            bg = 2.0 * bend * u3
            k0[n] += s * g0 + 2.0 * (slope * u1 + bg * p0)
            k1[n] += t * g0 + 2.0 * (slope * u2 + bg * p1)
            k2[n] += g0
        return tuple(k0), tuple(k1), tuple(k2)

    entry_i = lax.fori_loop(0, points // TILE, inner_entry, (blank, blank, blank))
    back(gw_ref, 2, wl_ref[0], uw_ref)
    entry_w = (blank, blank, blank)
    for direction in range(2):
        def wall_entry(i, carry, direction=direction):
            rows = rows_of(i)
            k0, k1, k2 = (list(part) for part in carry)
            s, t = sw_ref[rows, :], tw_ref[rows, :]
            for n, c in enumerate(spans):
                a = a0w_ref[rows, c]
                p = 2.0 * win_ref[direction, :, c]
                u0, u1 = uw_ref[0, rows, c], uw_ref[1, rows, c]
                slope = 1.0 - a * a
                g0 = slope * (u0 - 2.0 * a * (u1 * p))
                along = 2.0 * (slope * u1)
                k0[n] += s * g0 + along if direction == 0 else s * g0
                k1[n] += t * g0 + along if direction == 1 else t * g0
                k2[n] += g0
            return tuple(k0), tuple(k1), tuple(k2)

        tiles = rims // (2 * TILE)
        entry_w = lax.fori_loop(direction * tiles, (direction + 1) * tiles, wall_entry, entry_w)
    parts_ref[3:4, :] = biases_ref[0:1, :]
    parts_ref[7:8, :] = biases_ref[1:2, :]
    for k in range(3):
        for c, ei, ew in zip(spans, fold(entry_i[k]), fold(entry_w[k])):
            parts_ref[k : k + 1, c] = ei
            parts_ref[4 + k : 5 + k, c] = ew


def blend_kernel(
    inner_count, wall_count,
    sums_ref, parts_ref, isums_ref, wheads_ref, x0i_ref, gi_ref, x0w_ref, gw_ref,
    in_ref, local_ref, bias_ref, head_ref, tbias_ref, loss_ref,
):
    count, points, width = x0i_ref.shape
    rims = x0w_ref.shape[1]
    fr, fb, loss = factors(sums_ref[2:3, :], sums_ref[3:4, :], inner_count, wall_count)
    loss_ref[...] = loss[:, 0:1]
    tbias_ref[...] = fr * sums_ref[0:1, :] + fb * sums_ref[1:2, :]
    head_ref[...] = fr * isums_ref[1:2, :] + fb * wheads_ref[...]
    for k in range(3):
        in_ref[k] = fr * parts_ref[k : k + 1, :] + fb * parts_ref[4 + k : 5 + k, :]
    bias_ref[...] = fr * parts_ref[3:4, :] + fb * parts_ref[7:8, :]
    local_ref[0] = fr * tn(
        x0i_ref[...].reshape(count * points, width), gi_ref[...].reshape(count * points, width)
    ) + fb * tn(x0w_ref[...].reshape(2 * rims, width), gw_ref[...].reshape(2 * rims, width))


def call(kernel, outs, scratch, args, flops, space=pltpu.VMEM):
    vmem = pl.BlockSpec(memory_space=pltpu.VMEM)
    return pl.pallas_call(
        kernel,
        out_shape=outs,
        in_specs=[pl.BlockSpec(memory_space=space)] * len(args),
        out_specs=jax.tree.map(lambda _: vmem, outs),
        scratch_shapes=scratch,
        compiler_params=pltpu.CompilerParams(vmem_limit_bytes=20 << 20),
        cost_estimate=pl.CostEstimate(flops=flops, bytes_accessed=0, transcendentals=0),
    )(*args)


def shape(*dims, dtype=F32):
    return jax.ShapeDtypeStruct(dims, dtype)


def swap(x, axis, bit):
    return exchange(x, axis, 1 << bit)


def exchange(x, axis, mask):
    return lax.ppermute(x, axis, [(i, i ^ mask) for i in range(lax.axis_size(axis))])


def bits_of(axis):
    return [(axis, bit) for bit in range(lax.axis_size(axis).bit_length() - 1)]


def neighbours(lower, upper, axis):
    size = lax.axis_size(axis)
    even = lax.axis_index(axis) % 2 == 0
    within, across = [], []
    for i in range(0, size, 2):
        within += [(i, i + 1), (i + 1, i)]
        across += [(i + 1, (i + 2) % size), ((i + 2) % size, i + 1)]
    far = lax.ppermute(jnp.where(even, lower, upper), axis, across)
    close = lax.ppermute(jnp.where(even, upper, lower), axis, within)
    return jnp.where(even, far, close), jnp.where(even, close, far)


def together(*xs):
    return lax.optimization_barrier(xs)


def per_device(
    collocation, source, wall_index, bc_type, bc_value,
    in_weight, local_weight, local_bias, trunk_weight, trunk_bias, head_weight,
):
    rows, cols = lax.axis_size("sx"), lax.axis_size("sy")
    assert rows & (rows - 1) == 0 and cols & (cols - 1) == 0 and rows >= 4 and cols >= 2
    points, edge, width = collocation.shape[2], wall_index.shape[2], local_weight.shape[1]
    rims_total = 4 * edge
    inner_count = float(points * rows * cols)
    wall_count = float(rims_total * rows * cols)

    core = ("sy", 0)
    halved = (("sx", 0), ("sx", 1), core)
    doubled = [b for b in bits_of("sy") + bits_of("sx") if b not in halved]
    order_size = 1 << len(halved)

    def mine():
        return sum(((lax.axis_index(axis) >> bit) & 1) << k for k, (axis, bit) in enumerate(halved))

    big = shape(width, width)
    small = shape(8, width)

    def stack(count, size, dtype=F32):
        return shape(count, size, width, dtype=dtype)

    def vm(s):
        return pltpu.VMEM(s.shape, s.dtype)

    entry_weight = jnp.transpose(in_weight, (1, 0, 2))
    firsts = (wall_index, entry_weight, local_weight, local_bias, trunk_weight, trunk_bias, head_weight)
    (rims, sw, tw, a0w, x0w, z1w, x1w, z2w) = call(
        wall_forward_kernel,
        (
            shape(4, 2 * edge), shape(rims_total, LANES), shape(rims_total, LANES),
            shape(rims_total, width), stack(2, rims_total, BF16), stack(2, rims_total),
            stack(2, rims_total, BF16), stack(2, rims_total),
        ),
        [pltpu.VMEM((rims_total, LANES), F32)] * 2
        + [pltpu.SemaphoreType.DMA((len(firsts),))]
        + [vm(x) for x in firsts],
        tuple(pltpu.with_memory_space_constraint(x, pltpu.HBM) for x in firsts),
        4 * rims_total * 2 * width * width,
        pltpu.HBM,
    )
    south, north = neighbours(rims[2:3], rims[3:4], "sy")
    west, east = neighbours(rims[0:1], rims[1:2], "sx")

    (grad_r, isums, si, ti, a0i, x0i, z1i, g2i) = call(
        functools.partial(inner_kernel, order_size, mine),
        (
            big, small, shape(points, LANES), shape(points, LANES), shape(points, width),
            stack(5, points, BF16), stack(5, points), stack(5, points, BF16),
        ),
        [vm(stack(5, points, BF16)), vm(stack(5, points)), pltpu.VMEM((points, LANES), F32)],
        (collocation, source, entry_weight, local_weight, local_bias, trunk_weight, trunk_bias, head_weight),
        6 * points * 5 * width * width,
    )
    (grad_b, sums, wheads, g2w) = call(
        functools.partial(wall_top_kernel, order_size, mine, rows),
        (big, small, shape(1, width), stack(2, rims_total, BF16)),
        [pltpu.VMEM((rims_total, LANES), F32)] * 2,
        (rims, west, east, south, north, bc_type.T, bc_value, z2w, x1w, head_weight, isums),
        2 * rims_total * 2 * width * width,
    )
    half = width // 2
    got_r = swap(grad_r[half:], *core)
    grad_r = grad_r[:half] + got_r
    more = swap(sums, *core)
    sums = sums + more
    got_b = swap(grad_b[half:], *core)
    grad_b = grad_b[:half] + got_b
    part = half // 4
    gots = []
    for mask in (1, 2, 3):
        where = slice(mask * part, (mask + 1) * part)
        pair = []
        for x in (sums, jnp.concatenate([grad_r[where], grad_b[where]], axis=0)):
            pair.append(exchange(x, "sx", mask))
        gots.append(pair)
    sums = sums + gots[0][0] + gots[1][0] + gots[2][0]
    both = gots[0][1] + gots[1][1] + gots[2][1]
    keep_r = grad_r[:part] + both[:part]
    keep_b = grad_b[:part] + both[part:]
    sums, g2w = together(sums, g2w)
    for axis, bit in doubled:
        more = swap(sums, axis, bit)
        sums = sums + more
    gi, gw, biases = call(
        hidden_kernel,
        (stack(5, points, BF16), stack(2, rims_total, BF16), small),
        [vm(stack(4, points)), vm(stack(2, rims_total))],
        (trunk_weight, z1i, g2i, z1w, g2w),
        2 * (points * 4 + rims_total * 2) * width * width,
    )
    fr, fb, _ = factors(sums[2:3], sums[3:4], inner_count, wall_count)
    block = fr * keep_r + fb * keep_b
    block, biases = together(block, biases)
    for axis, bit in doubled[:1]:
        block = block + swap(block, axis, bit)
    parts = call(
        entry_kernel,
        small,
        [vm(stack(4, points)), vm(stack(2, rims_total))],
        (entry_weight, local_weight, si, ti, a0i, gi, sw, tw, a0w, gw, biases),
        2 * (points * 4 + rims_total * 2) * width * width,
    )
    block, parts = together(block, parts)
    for axis, bit in doubled[1:]:
        block = block + swap(block, axis, bit)
    in_grad, local_grad, local_bias_grad, head_grad, trunk_bias_grad, loss = call(
        functools.partial(blend_kernel, inner_count, wall_count),
        (shape(3, 1, width), shape(1, width, width)) + (shape(1, width),) * 3 + (shape(1, 1),),
        [],
        (sums, parts, isums, wheads, x0i, gi, x0w, gw),
        2 * (points * 5 + rims_total * 2) * width * width,
    )
    blocks = [block]
    for mask in (1, 2, 3):
        blocks.append(exchange(block, "sx", mask))
    *blocks, local_bias_grad = together(*blocks, local_bias_grad)
    blocks = blocks + [swap(b, *core) for b in blocks]
    trunk_grad = call(
        functools.partial(unorder_kernel, order_size, mine),
        shape(1, width, width),
        [],
        tuple(blocks),
        width * width,
    )
    return (
        trunk_grad, trunk_bias_grad, jnp.transpose(in_grad, (1, 0, 2)), local_grad,
        local_bias_grad, head_grad, loss.reshape(()),
    )


def solution(mesh):
    return jax.shard_map(
        per_device,
        mesh=mesh,
        in_specs=(
            P(None, "sx", "sy"),
            P("sx", "sy"),
            P(None, "sx", "sy"),
            P(None, "sy"),
            P(None, "sy"),
            P("sx", None, "sy"),
            P("sx", None, "sy"),
            P("sx", "sy"),
            P(),
            P(),
            P("sx", "sy"),
        ),
        out_specs=(
            P(),
            P(),
            P("sx", None, "sy"),
            P("sx", None, "sy"),
            P("sx", "sy"),
            P("sx", "sy"),
            P(),
        ),
        check_vma=False,
    )
```

```python
import functools

import jax
import jax.numpy as jnp
from jax import lax
from jax.experimental import pallas as pl
from jax.experimental.pallas import tpu as pltpu
from jax.sharding import PartitionSpec as P


SLOTS = 1024
EPS = 1e-06
TILE = 16
LANES = 128
F32 = jnp.float32
BF16 = jnp.bfloat16


def nn(a, b):
    return lax.dot_general(a, b, (((1,), (0,)), ((), ())), preferred_element_type=F32)


def nt(a, b):
    return lax.dot_general(a, b, (((1,), (1,)), ((), ())), preferred_element_type=F32)


def tn(a, b):
    return lax.dot_general(a, b, (((0,), (0,)), ((), ())), preferred_element_type=F32)


def eye_mask(rows, cols, shift=0):
    r = lax.broadcasted_iota(jnp.int32, (rows, cols), 0)
    c = lax.broadcasted_iota(jnp.int32, (rows, cols), 1)
    return r + shift == c


def to_column(row):
    size = row.shape[1]
    return jnp.sum(jnp.where(eye_mask(size, size), row, 0.0), axis=1, keepdims=True)


def chunks(width):
    return [slice(k, k + LANES) for k in range(0, width, LANES)]


def fold(parts):
    return [jnp.sum(p, axis=0, keepdims=True) for p in parts]


def zeros_tile():
    return jnp.zeros((TILE, LANES), F32)


def rows_of(i):
    return pl.ds(pl.multiple_of(i * TILE, TILE), TILE)


def wall_columns(index_ref, s_ref, t_ref):
    edge = index_ref.shape[2]
    shape = (edge, LANES)
    for w in range(4):
        spots = (2.0 * index_ref[w].astype(F32) + 1.0) / SLOTS - 1.0
        moving = jnp.broadcast_to(to_column(spots), shape)
        fixed = jnp.full(shape, -1.0 if w % 2 == 0 else 1.0, F32)
        where = pl.ds(w * edge, edge)
        s_ref[where, :] = fixed if w < 2 else moving
        t_ref[where, :] = moving if w < 2 else fixed


def wall_forward_kernel(*refs):
    far, refs = refs[:7], refs[7:]
    (rims_ref, s_ref, t_ref, a0_ref, x0_ref, z1_ref, x1_ref, z2_ref), refs = refs[:8], refs[8:]
    ua_ref, da_ref, sems = refs[:3]
    near = refs[3:]
    copies = [pltpu.make_async_copy(f, n, sems.at[k]) for k, (f, n) in enumerate(zip(far, near))]
    index_ref, win_ref, wl_ref, bl_ref, wt_ref, bt_ref, head_ref = near
    for copy in copies:
        copy.start()
    edge = index_ref.shape[2]
    points, width = a0_ref.shape
    copies[0].wait()
    copies[1].wait()
    wall_columns(index_ref, s_ref, t_ref)

    for direction in range(2):
        def entry(i, carry, direction=direction):
            rows = rows_of(i)
            s, t = s_ref[rows, :], t_ref[rows, :]
            for c in chunks(width):
                w0, w1, wb = (win_ref[k, :, c] for k in range(3))
                a = jnp.tanh(s * w0 + t * w1 + wb)
                slope = 1.0 - a * a
                a0_ref[rows, c] = a
                x0_ref[0, rows, c] = a.astype(BF16)
                x0_ref[1, rows, c] = (slope * (2.0 * (w0, w1)[direction])).astype(BF16)
            return carry

        tiles = points // (2 * TILE)
        lax.fori_loop(direction * tiles, (direction + 1) * tiles, entry, 0, unroll=2)

    for copy in copies[2:]:
        copy.wait()
    z1_ref[...] = nn(x0_ref[...].reshape(2 * points, width), wl_ref[0]).reshape(2, points, width)

    def hidden(i, carry):
        rows = rows_of(i)
        for c in chunks(width):
            a = jnp.tanh(z1_ref[0, rows, c] + bl_ref[:, c])
            slope = 1.0 - a * a
            z1_ref[0, rows, c] = a
            x1_ref[0, rows, c] = a.astype(BF16)
            x1_ref[1, rows, c] = (slope * z1_ref[1, rows, c]).astype(BF16)
        return carry

    lax.fori_loop(0, points // TILE, hidden, 0, unroll=2)
    z2_ref[...] = nn(x1_ref[...].reshape(2 * points, width), wt_ref[0]).reshape(2, points, width)

    def final(i, carry):
        rows = rows_of(i)
        u, d = zeros_tile(), zeros_tile()
        for c in chunks(width):
            a = jnp.tanh(z2_ref[0, rows, c] + bt_ref[:, c])
            slope = 1.0 - a * a
            z2_ref[0, rows, c] = a
            u += a * head_ref[:, c]
            d += slope * z2_ref[1, rows, c] * head_ref[:, c]
        ua_ref[rows, :] = u
        da_ref[rows, :] = d
        return carry

    lax.fori_loop(0, points // TILE, final, 0, unroll=2)
    value = jnp.sum(ua_ref[...], axis=1, keepdims=True)
    slope = jnp.sum(da_ref[...], axis=1, keepdims=True)
    low, high = eye_mask(edge, 2 * edge), eye_mask(edge, 2 * edge, edge)
    for w in range(4):
        part = slice(w * edge, (w + 1) * edge)
        both = jnp.where(low, value[part], 0.0) + jnp.where(high, slope[part], 0.0)
        rims_ref[w : w + 1, :] = jnp.sum(both, axis=0, keepdims=True)


def inner_kernel(
    order_size, order_of,
    points_ref, source_ref, win_ref, wl_ref, bl_ref, wt_ref, bt_ref, head_ref,
    grad_ref, sums_ref, s_ref, t_ref, a0_ref, x0_ref, z1_ref, g2_ref,
    x1_ref, z2_ref, acc_ref,
):
    points, width = a0_ref.shape
    for k in range(0, points, LANES):
        where = pl.ds(k, LANES)
        for ref, which in ((s_ref, 0), (t_ref, 1)):
            column = to_column(points_ref[which, :, k : k + LANES])
            ref[where, :] = jnp.broadcast_to(column, (LANES, LANES))

    def entry(i, carry):
        rows = rows_of(i)
        s, t = s_ref[rows, :], t_ref[rows, :]
        for c in chunks(width):
            w0, w1, wb = (win_ref[k, :, c] for k in range(3))
            p0, p1 = 2.0 * w0, 2.0 * w1
            a = jnp.tanh(s * w0 + t * w1 + wb)
            slope = 1.0 - a * a
            bend = -2.0 * a * slope
            a0_ref[rows, c] = a
            x0_ref[0, rows, c] = a.astype(BF16)
            x0_ref[1, rows, c] = (slope * p0).astype(BF16)
            x0_ref[2, rows, c] = (slope * p1).astype(BF16)
            x0_ref[3, rows, c] = (bend * (p0 * p0)).astype(BF16)
            x0_ref[4, rows, c] = (bend * (p1 * p1)).astype(BF16)
        return carry

    tiles = points // TILE
    lax.fori_loop(0, tiles, entry, 0, unroll=2)
    z1_ref[...] = nn(x0_ref[...].reshape(5 * points, width), wl_ref[0]).reshape(5, points, width)

    def hidden(i, carry):
        rows = rows_of(i)
        for c in chunks(width):
            a = jnp.tanh(z1_ref[0, rows, c] + bl_ref[:, c])
            p0, p1 = z1_ref[1, rows, c], z1_ref[2, rows, c]
            slope = 1.0 - a * a
            bend = -2.0 * a * slope
            z1_ref[0, rows, c] = a
            x1_ref[0, rows, c] = a.astype(BF16)
            x1_ref[1, rows, c] = (slope * p0).astype(BF16)
            x1_ref[2, rows, c] = (slope * p1).astype(BF16)
            x1_ref[3, rows, c] = (slope * z1_ref[3, rows, c] + bend * p0 * p0).astype(BF16)
            x1_ref[4, rows, c] = (slope * z1_ref[4, rows, c] + bend * p1 * p1).astype(BF16)
        return carry

    lax.fori_loop(0, tiles, hidden, 0, unroll=2)
    z2_ref[...] = nn(x1_ref[...].reshape(5 * points, width), wt_ref[0]).reshape(5, points, width)

    def final(i, carry):
        rows = rows_of(i)
        total = zeros_tile()
        for c in chunks(width):
            a = jnp.tanh(z2_ref[0, rows, c] + bt_ref[:, c])
            p0, p1 = z2_ref[1, rows, c], z2_ref[2, rows, c]
            slope = 1.0 - a * a
            bend = -2.0 * a * slope
            second = z2_ref[3, rows, c] + z2_ref[4, rows, c]
            bent = slope * second + bend * (p0 * p0 + p1 * p1)
            z2_ref[0, rows, c] = a
            z2_ref[3, rows, c] = second
            z2_ref[4, rows, c] = bent
            total += bent * head_ref[:, c]
        acc_ref[rows, :] = total
        return carry

    lax.fori_loop(0, tiles, final, 0, unroll=2)
    residual = jnp.sum(acc_ref[...], axis=1, keepdims=True)
    forcing = [to_column(source_ref[:, k : k + LANES]) for k in range(0, points, LANES)]
    residual = residual + jnp.concatenate(forcing, axis=0)
    acc_ref[...] = jnp.broadcast_to(2.0 * residual, acc_ref.shape)
    square = jnp.sum(residual * residual, axis=0, keepdims=True)

    spans = chunks(width)

    def top(i, carry):
        rows = rows_of(i)
        heads, biases = list(carry[0]), list(carry[1])
        twice = acc_ref[rows, :]
        for n, c in enumerate(spans):
            a = z2_ref[0, rows, c]
            p0, p1 = z2_ref[1, rows, c], z2_ref[2, rows, c]
            slope = 1.0 - a * a
            bend = -2.0 * a * slope
            g = twice * head_ref[:, c]
            heads[n] += twice * z2_ref[4, rows, c]
            gc = g * (p0 * p0 + p1 * p1)
            gs = g * z2_ref[3, rows, c] - 2.0 * a * gc
            g0 = slope * (-2.0 * (gc * slope + gs * a))
            bg = 2.0 * bend * g
            g3 = (slope * g).astype(BF16)
            biases[n] += g0
            g2_ref[0, rows, c] = g0.astype(BF16)
            g2_ref[1, rows, c] = (bg * p0).astype(BF16)
            g2_ref[2, rows, c] = (bg * p1).astype(BF16)
            g2_ref[3, rows, c] = g3
            g2_ref[4, rows, c] = g3
        return tuple(heads), tuple(biases)

    blank = tuple(zeros_tile() for _ in spans)
    heads, biases = lax.fori_loop(0, tiles, top, (blank, blank))
    sums_ref[...] = jnp.zeros(sums_ref.shape, F32)
    for c, hp, bp in zip(spans, fold(heads), fold(biases)):
        sums_ref[0:1, c] = bp
        sums_ref[1:2, c] = hp
    sums_ref[2:3, :] = jnp.broadcast_to(square, (1, width))
    store_ordered(
        grad_ref,
        tn(x1_ref[...].reshape(5 * points, width), g2_ref[...].reshape(5 * points, width)),
        order_size, order_of,
    )


def store_ordered(grad_ref, grad, order_size, order_of):
    mine = order_of()
    size = grad.shape[0] // order_size
    for block in range(order_size):
        where = pl.ds(pl.multiple_of((mine ^ block) * size, size), size)
        grad_ref[where, :] = grad[block * size : (block + 1) * size]


def wall_top_kernel(
    order_size, order_of, row_size,
    rims_ref, west_ref, east_ref, south_ref, north_ref, type_ref, value_ref,
    z2_ref, x1_ref, head_ref, isums_ref,
    grad_ref, sums_ref, heads_ref, g2_ref,
    cu_ref, cd_ref,
):
    _, points, width = z2_ref.shape
    edge = points // 4
    place = lax.axis_index("sx")
    outer = (place == 0, place == row_size - 1)
    low, high = eye_mask(edge, 2 * edge), eye_mask(edge, 2 * edge, edge)
    total = jnp.zeros((1, 1), F32)

    def split(row):
        u = jnp.sum(jnp.where(low, row, 0.0), axis=1, keepdims=True)
        d = jnp.sum(jnp.where(high, row, 0.0), axis=1, keepdims=True)
        return u, d

    for w, near in enumerate((west_ref, east_ref, south_ref, north_ref)):
        u, d = split(rims_ref[w : w + 1, :])
        un, dn = split(near[...])
        eu, ed = u - un, d - dn
        if w < 2:
            normal = -1.0 if w == 0 else 1.0
            g = to_column(value_ref[w : w + 1, :])
            fixed = type_ref[:, w : w + 1] == 0
            bu = jnp.where(fixed, u - g, 0.0)
            bd = jnp.where(fixed, 0.0, normal * (normal * d - g))
            eu = jnp.where(outer[w], bu, eu)
            ed = jnp.where(outer[w], bd, ed)
        total += jnp.sum(eu * eu + ed * ed, axis=0, keepdims=True)
        where = pl.ds(w * edge, edge)
        cu_ref[where, :] = jnp.broadcast_to(2.0 * eu, (edge, LANES))
        cd_ref[where, :] = jnp.broadcast_to(2.0 * ed, (edge, LANES))

    spans = chunks(width)

    def top(i, carry):
        rows = rows_of(i)
        heads, biases = list(carry[0]), list(carry[1])
        cu, cd = cu_ref[rows, :], cd_ref[rows, :]
        for n, c in enumerate(spans):
            a, p = z2_ref[0, rows, c], z2_ref[1, rows, c]
            slope = 1.0 - a * a
            h = head_ref[:, c]
            gv, gd = cu * h, cd * h
            heads[n] += cu * a + cd * (slope * p)
            g0 = slope * (gv - 2.0 * a * (gd * p))
            biases[n] += g0
            g2_ref[0, rows, c] = g0.astype(BF16)
            g2_ref[1, rows, c] = (slope * gd).astype(BF16)
        return tuple(heads), tuple(biases)

    blank = tuple(zeros_tile() for _ in spans)
    heads, biases = lax.fori_loop(0, points // TILE, top, (blank, blank))
    sums_ref[...] = jnp.zeros(sums_ref.shape, F32)
    for c, hp, bp in zip(spans, fold(heads), fold(biases)):
        sums_ref[1:2, c] = bp
        heads_ref[:, c] = hp
    sums_ref[0:1, :] = isums_ref[0:1, :]
    sums_ref[2:3, :] = isums_ref[2:3, :]
    sums_ref[3:4, :] = jnp.broadcast_to(total, (1, width))
    store_ordered(
        grad_ref,
        tn(x1_ref[...].reshape(2 * points, width), g2_ref[...].reshape(2 * points, width)),
        order_size, order_of,
    )


def factors(total_r, total_b, inner_count, wall_count):
    mean_r = total_r / inner_count
    mean_b = total_b / wall_count
    lam = jnp.sqrt((mean_b + EPS) / (mean_r + EPS))
    return lam / inner_count, 1.0 / wall_count, lam * mean_r + mean_b


def unorder_kernel(order_size, order_of, *refs):
    ins, out_ref, sems = refs[:order_size], refs[order_size], refs[order_size + 1]
    size = ins[0].shape[0]
    mine = order_of()
    copies = []
    for place, ref in enumerate(ins):
        where = pl.ds(pl.multiple_of((mine ^ place) * size, size), size)
        copies.append(pltpu.make_async_copy(ref, out_ref.at[0, where, :], sems.at[place]))
    for copy in copies:
        copy.start()
    for copy in copies:
        copy.wait()


def back(g_ref, count, weight, u_ref):
    _, size, width = g_ref.shape
    flat = g_ref[0:count].reshape(count * size, width)
    u_ref[...] = nt(flat, weight).reshape(count, size, width)


def hidden_kernel(
    wt_ref, z1i_ref, g2i_ref, z1w_ref, g2w_ref,
    gi_ref, gw_ref, biases_ref,
    ui_ref, uw_ref,
):
    _, points, width = z1i_ref.shape
    rims = z1w_ref.shape[1]
    spans = chunks(width)
    blank = tuple(zeros_tile() for _ in spans)

    back(g2i_ref, 4, wt_ref[0], ui_ref)

    def inner_hidden(i, carry):
        rows = rows_of(i)
        biases = list(carry)
        for n, c in enumerate(spans):
            a, p0, p1 = z1i_ref[0, rows, c], z1i_ref[1, rows, c], z1i_ref[2, rows, c]
            u0, u1, u2, u3 = (ui_ref[k, rows, c] for k in range(4))
            slope = 1.0 - a * a
            bend = -2.0 * a * slope
            gc = u3 * (p0 * p0 + p1 * p1)
            second = z1i_ref[3, rows, c] + z1i_ref[4, rows, c]
            gs = u1 * p0 + u2 * p1 + u3 * second - 2.0 * a * gc
            g0 = slope * (u0 - 2.0 * (gc * slope + gs * a))
            bg = 2.0 * bend * u3
            g3 = (slope * u3).astype(BF16)
            biases[n] += g0
            gi_ref[0, rows, c] = g0.astype(BF16)
            gi_ref[1, rows, c] = (slope * u1 + bg * p0).astype(BF16)
            gi_ref[2, rows, c] = (slope * u2 + bg * p1).astype(BF16)
            gi_ref[3, rows, c] = g3
            gi_ref[4, rows, c] = g3
        return tuple(biases)

    bias_i = lax.fori_loop(0, points // TILE, inner_hidden, blank)
    back(g2w_ref, 2, wt_ref[0], uw_ref)

    def wall_hidden(i, carry):
        rows = rows_of(i)
        biases = list(carry)
        for n, c in enumerate(spans):
            a, p = z1w_ref[0, rows, c], z1w_ref[1, rows, c]
            u0, u1 = uw_ref[0, rows, c], uw_ref[1, rows, c]
            slope = 1.0 - a * a
            g0 = slope * (u0 - 2.0 * a * (u1 * p))
            biases[n] += g0
            gw_ref[0, rows, c] = g0.astype(BF16)
            gw_ref[1, rows, c] = (slope * u1).astype(BF16)
        return tuple(biases)

    bias_w = lax.fori_loop(0, rims // TILE, wall_hidden, blank)
    biases_ref[...] = jnp.zeros(biases_ref.shape, F32)
    for c, bi, bw in zip(spans, fold(bias_i), fold(bias_w)):
        biases_ref[0:1, c] = bi
        biases_ref[1:2, c] = bw


def entry_kernel(
    win_ref, wl_ref,
    si_ref, ti_ref, a0i_ref, gi_ref, sw_ref, tw_ref, a0w_ref, gw_ref, biases_ref,
    parts_ref,
    ui_ref, uw_ref,
):
    points, width = a0i_ref.shape
    rims = a0w_ref.shape[0]
    spans = chunks(width)
    blank = tuple(zeros_tile() for _ in spans)
    back(gi_ref, 4, wl_ref[0], ui_ref)

    def inner_entry(i, carry):
        rows = rows_of(i)
        k0, k1, k2 = (list(part) for part in carry)
        s, t = si_ref[rows, :], ti_ref[rows, :]
        for n, c in enumerate(spans):
            a = a0i_ref[rows, c]
            p0, p1 = 2.0 * win_ref[0, :, c], 2.0 * win_ref[1, :, c]
            u0, u1, u2, u3 = (ui_ref[k, rows, c] for k in range(4))
            slope = 1.0 - a * a
            bend = -2.0 * a * slope
            gc = u3 * (p0 * p0 + p1 * p1)
            gs = u1 * p0 + u2 * p1 - 2.0 * a * gc
            g0 = slope * (u0 - 2.0 * (gc * slope + gs * a))
            bg = 2.0 * bend * u3
            k0[n] += s * g0 + 2.0 * (slope * u1 + bg * p0)
            k1[n] += t * g0 + 2.0 * (slope * u2 + bg * p1)
            k2[n] += g0
        return tuple(k0), tuple(k1), tuple(k2)

    entry_i = lax.fori_loop(0, points // TILE, inner_entry, (blank, blank, blank))
    back(gw_ref, 2, wl_ref[0], uw_ref)
    entry_w = (blank, blank, blank)
    for direction in range(2):
        def wall_entry(i, carry, direction=direction):
            rows = rows_of(i)
            k0, k1, k2 = (list(part) for part in carry)
            s, t = sw_ref[rows, :], tw_ref[rows, :]
            for n, c in enumerate(spans):
                a = a0w_ref[rows, c]
                p = 2.0 * win_ref[direction, :, c]
                u0, u1 = uw_ref[0, rows, c], uw_ref[1, rows, c]
                slope = 1.0 - a * a
                g0 = slope * (u0 - 2.0 * a * (u1 * p))
                along = 2.0 * (slope * u1)
                k0[n] += s * g0 + along if direction == 0 else s * g0
                k1[n] += t * g0 + along if direction == 1 else t * g0
                k2[n] += g0
            return tuple(k0), tuple(k1), tuple(k2)

        tiles = rims // (2 * TILE)
        entry_w = lax.fori_loop(direction * tiles, (direction + 1) * tiles, wall_entry, entry_w)
    parts_ref[3:4, :] = biases_ref[0:1, :]
    parts_ref[7:8, :] = biases_ref[1:2, :]
    for k in range(3):
        for c, ei, ew in zip(spans, fold(entry_i[k]), fold(entry_w[k])):
            parts_ref[k : k + 1, c] = ei
            parts_ref[4 + k : 5 + k, c] = ew


def blend_kernel(
    inner_count, wall_count,
    sums_ref, parts_ref, isums_ref, wheads_ref, x0i_ref, gi_ref, x0w_ref, gw_ref,
    in_ref, local_ref, bias_ref, head_ref, tbias_ref, loss_ref,
):
    count, points, width = x0i_ref.shape
    rims = x0w_ref.shape[1]
    fr, fb, loss = factors(sums_ref[2:3, :], sums_ref[3:4, :], inner_count, wall_count)
    loss_ref[...] = loss[:, 0:1]
    tbias_ref[...] = fr * sums_ref[0:1, :] + fb * sums_ref[1:2, :]
    head_ref[...] = fr * isums_ref[1:2, :] + fb * wheads_ref[...]
    for k in range(3):
        in_ref[k] = fr * parts_ref[k : k + 1, :] + fb * parts_ref[4 + k : 5 + k, :]
    bias_ref[...] = fr * parts_ref[3:4, :] + fb * parts_ref[7:8, :]
    local_ref[0] = fr * tn(
        x0i_ref[...].reshape(count * points, width), gi_ref[...].reshape(count * points, width)
    ) + fb * tn(x0w_ref[...].reshape(2 * rims, width), gw_ref[...].reshape(2 * rims, width))


def call(kernel, outs, scratch, args, flops, space=pltpu.VMEM, into=pltpu.VMEM):
    vmem = pl.BlockSpec(memory_space=into)
    return pl.pallas_call(
        kernel,
        out_shape=outs,
        in_specs=[pl.BlockSpec(memory_space=space)] * len(args),
        out_specs=jax.tree.map(lambda _: vmem, outs),
        scratch_shapes=scratch,
        compiler_params=pltpu.CompilerParams(vmem_limit_bytes=20 << 20),
        cost_estimate=pl.CostEstimate(flops=flops, bytes_accessed=0, transcendentals=0),
    )(*args)


def shape(*dims, dtype=F32):
    return jax.ShapeDtypeStruct(dims, dtype)


def swap(x, axis, bit):
    return exchange(x, axis, 1 << bit)


def exchange(x, axis, mask):
    return lax.ppermute(x, axis, [(i, i ^ mask) for i in range(lax.axis_size(axis))])


def bits_of(axis):
    return [(axis, bit) for bit in range(lax.axis_size(axis).bit_length() - 1)]


def neighbours(lower, upper, axis):
    size = lax.axis_size(axis)
    even = lax.axis_index(axis) % 2 == 0
    within, across = [], []
    for i in range(0, size, 2):
        within += [(i, i + 1), (i + 1, i)]
        across += [(i + 1, (i + 2) % size), ((i + 2) % size, i + 1)]
    far = lax.ppermute(jnp.where(even, lower, upper), axis, across)
    close = lax.ppermute(jnp.where(even, upper, lower), axis, within)
    return jnp.where(even, far, close), jnp.where(even, close, far)


def together(*xs):
    return lax.optimization_barrier(xs)


def per_device(
    collocation, source, wall_index, bc_type, bc_value,
    in_weight, local_weight, local_bias, trunk_weight, trunk_bias, head_weight,
):
    rows, cols = lax.axis_size("sx"), lax.axis_size("sy")
    assert rows & (rows - 1) == 0 and cols & (cols - 1) == 0 and rows >= 4 and cols >= 2
    points, edge, width = collocation.shape[2], wall_index.shape[2], local_weight.shape[1]
    rims_total = 4 * edge
    inner_count = float(points * rows * cols)
    wall_count = float(rims_total * rows * cols)

    core = ("sy", 0)
    halved = (("sx", 0), ("sx", 1), core)
    doubled = [b for b in bits_of("sy") + bits_of("sx") if b not in halved]
    order_size = 1 << len(halved)

    def mine():
        return sum(((lax.axis_index(axis) >> bit) & 1) << k for k, (axis, bit) in enumerate(halved))

    big = shape(width, width)
    small = shape(8, width)

    def stack(count, size, dtype=F32):
        return shape(count, size, width, dtype=dtype)

    def vm(s):
        return pltpu.VMEM(s.shape, s.dtype)

    entry_weight = jnp.transpose(in_weight, (1, 0, 2))
    firsts = (wall_index, entry_weight, local_weight, local_bias, trunk_weight, trunk_bias, head_weight)
    (rims, sw, tw, a0w, x0w, z1w, x1w, z2w) = call(
        wall_forward_kernel,
        (
            shape(4, 2 * edge), shape(rims_total, LANES), shape(rims_total, LANES),
            shape(rims_total, width), stack(2, rims_total, BF16), stack(2, rims_total),
            stack(2, rims_total, BF16), stack(2, rims_total),
        ),
        [pltpu.VMEM((rims_total, LANES), F32)] * 2
        + [pltpu.SemaphoreType.DMA((len(firsts),))]
        + [vm(x) for x in firsts],
        tuple(pltpu.with_memory_space_constraint(x, pltpu.HBM) for x in firsts),
        4 * rims_total * 2 * width * width,
        pltpu.HBM,
    )
    south, north = neighbours(rims[2:3], rims[3:4], "sy")
    west, east = neighbours(rims[0:1], rims[1:2], "sx")

    (grad_r, isums, si, ti, a0i, x0i, z1i, g2i) = call(
        functools.partial(inner_kernel, order_size, mine),
        (
            big, small, shape(points, LANES), shape(points, LANES), shape(points, width),
            stack(5, points, BF16), stack(5, points), stack(5, points, BF16),
        ),
        [vm(stack(5, points, BF16)), vm(stack(5, points)), pltpu.VMEM((points, LANES), F32)],
        (collocation, source, entry_weight, local_weight, local_bias, trunk_weight, trunk_bias, head_weight),
        6 * points * 5 * width * width,
    )
    (grad_b, sums, wheads, g2w) = call(
        functools.partial(wall_top_kernel, order_size, mine, rows),
        (big, small, shape(1, width), stack(2, rims_total, BF16)),
        [pltpu.VMEM((rims_total, LANES), F32)] * 2,
        (rims, west, east, south, north, bc_type.T, bc_value, z2w, x1w, head_weight, isums),
        2 * rims_total * 2 * width * width,
    )
    half = width // 2
    got_r = swap(grad_r[half:], *core)
    grad_r = grad_r[:half] + got_r
    more = swap(sums, *core)
    sums = sums + more
    got_b = swap(grad_b[half:], *core)
    grad_b = grad_b[:half] + got_b
    part = half // 4
    gots = []
    for mask in (1, 2, 3):
        where = slice(mask * part, (mask + 1) * part)
        pair = []
        for x in (sums, jnp.concatenate([grad_r[where], grad_b[where]], axis=0)):
            pair.append(exchange(x, "sx", mask))
        gots.append(pair)
    sums = sums + gots[0][0] + gots[1][0] + gots[2][0]
    both = gots[0][1] + gots[1][1] + gots[2][1]
    keep_r = grad_r[:part] + both[:part]
    keep_b = grad_b[:part] + both[part:]
    sums, g2w = together(sums, g2w)
    for axis, bit in doubled:
        more = swap(sums, axis, bit)
        sums = sums + more
    gi, gw, biases = call(
        hidden_kernel,
        (stack(5, points, BF16), stack(2, rims_total, BF16), small),
        [vm(stack(4, points)), vm(stack(2, rims_total))],
        (trunk_weight, z1i, g2i, z1w, g2w),
        2 * (points * 4 + rims_total * 2) * width * width,
    )
    fr, fb, _ = factors(sums[2:3], sums[3:4], inner_count, wall_count)
    block = fr * keep_r + fb * keep_b
    block, biases = together(block, biases)
    for axis, bit in doubled[:1]:
        block = block + swap(block, axis, bit)
    parts = call(
        entry_kernel,
        small,
        [vm(stack(4, points)), vm(stack(2, rims_total))],
        (entry_weight, local_weight, si, ti, a0i, gi, sw, tw, a0w, gw, biases),
        2 * (points * 4 + rims_total * 2) * width * width,
    )
    block, parts = together(block, parts)
    for axis, bit in doubled[1:]:
        block = block + swap(block, axis, bit)
    in_grad, local_grad, local_bias_grad, head_grad, trunk_bias_grad, loss = call(
        functools.partial(blend_kernel, inner_count, wall_count),
        (shape(3, 1, width), shape(1, width, width)) + (shape(1, width),) * 3 + (shape(1, 1),),
        [],
        (sums, parts, isums, wheads, x0i, gi, x0w, gw),
        2 * (points * 5 + rims_total * 2) * width * width,
    )
    blocks = [block]
    for mask in (1, 2, 3):
        blocks.append(exchange(block, "sx", mask))
    *blocks, local_bias_grad = together(*blocks, local_bias_grad)
    blocks = blocks + [swap(b, *core) for b in blocks]
    trunk_grad = call(
        functools.partial(unorder_kernel, order_size, mine),
        shape(1, width, width),
        [pltpu.SemaphoreType.DMA((order_size,))],
        tuple(blocks),
        width * width,
        into=pltpu.HBM,
    )
    return (
        trunk_grad, trunk_bias_grad, jnp.transpose(in_grad, (1, 0, 2)), local_grad,
        local_bias_grad, head_grad, loss.reshape(()),
    )


def solution(mesh):
    return jax.shard_map(
        per_device,
        mesh=mesh,
        in_specs=(
            P(None, "sx", "sy"),
            P("sx", "sy"),
            P(None, "sx", "sy"),
            P(None, "sy"),
            P(None, "sy"),
            P("sx", None, "sy"),
            P("sx", None, "sy"),
            P("sx", "sy"),
            P(),
            P(),
            P("sx", "sy"),
        ),
        out_specs=(
            P(),
            P(),
            P("sx", None, "sy"),
            P("sx", None, "sy"),
            P("sx", "sy"),
            P("sx", "sy"),
            P(),
        ),
        check_vma=False,
    )
```
